256 devices in a mesh: pipe: 2 (over x_hi), tensor: 8 (over y, core), seq: 16 (over z, x_lo).
Axes of the slice: x: 4 (x_hi: 2, x_lo: 2; x = x_hi * 2 + x_lo), y: 4, z: 8, core: 2. Of those that a mesh axis runs over, the one named last changes fastest.
Arguments:
- tokens: bfloat16 [2, 2048, 2560], P(None, 'seq', 'tensor'), may hold values from -6 to 6
- prenorm_gain: float32 [2, 2560], P('pipe'), may hold values from 0.5 to 1.5
- gate_weight: bfloat16 [2, 2560, 5120], P('pipe', None, 'tensor'), may hold values from -0.125 to 0.125
- inner_weight: bfloat16 [2, 2560, 5120], P('pipe', None, 'tensor'), may hold values from -0.125 to 0.125
- state_weight: bfloat16 [2, 2560, 256], P('pipe'), may hold values from -0.125 to 0.125
- step_weight: bfloat16 [2, 2560, 80], P('pipe', None, 'tensor'), may hold values from -0.125 to 0.125
- inner_taps: float32 [2, 5, 5120], P('pipe', None, 'tensor'), may hold values from -3 to 3
- state_taps: float32 [2, 5, 256], P('pipe'), may hold values from -3 to 3
- step_bias: float32 [2, 80], P('pipe', 'tensor'), may hold values from -5 to -2
- decay_rate: float32 [2, 80], P('pipe', 'tensor'), may hold values from 0.00048828125 to 1
- skip_scale: float32 [2, 80], P('pipe', 'tensor'), may hold values from 0.5 to 1.5
- inner_gain: float32 [2, 5120], P('pipe', 'tensor'), may hold values from 0.5 to 1.5
- out_weight: bfloat16 [2, 5120, 2560], P('pipe', 'tensor'), may hold values from -0.078125 to 0.078125
Outputs:
- layer_outputs: bfloat16 [2, 2, 2048, 2560], P('pipe', None, 'seq', 'tensor')
The draws below stay inside these ranges and needn't reach their ends.
All inputs are finite; a program needn't handle non-finite values.
Results may differ from the reference program's by a relative error of at most 0.019.
Values may be sent and summed in bfloat16 or wider, within the bound.
A program may use at most 64 MiB of HBM per device.

```python
import math
import jax
import jax.numpy as jnp
from jax import lax

D = 2560
HEADS = 80
HEADDIM = 64
STATE = 128
KW = 4
BLOCK = 128
MICRO = 2
INNER = 5120
TOKENS = 2048
LAYERS = 2


def block_levels(own_key, extent, cuts, least, top_value):
    level, own = 1.0, jax.random.fold_in(own_key, 6)
    for position, shards_of in cuts:
        steps = jnp.exp(jax.random.uniform(jax.random.fold_in(own, position), (shards_of,), jnp.float32, least / len(cuts), top_value / len(cuts)))
        level = level * jnp.repeat(steps, extent[position] // shards_of).reshape([-1 if axis == position else 1 for axis in range(len(extent))])
    return level


def gaussian(own_key, shape, scale, bound, shards=(), held_as=jnp.bfloat16):
    values = scale * jax.random.normal(own_key, shape, jnp.float32)
    if shards:
        values = values * block_levels(own_key, shape, shards, -0.22, 0.18)
    return jnp.clip(values, -bound, bound).astype(held_as)


def setup_inputs(seed: int = 0) -> dict:
    splits = jax.random.split(jax.random.key(seed), 14)
    return {
        "tokens": gaussian(splits[0], (MICRO, TOKENS, D), 1.0, 6.0, ((1, 16), (2, 8))),
        "prenorm_gain": jnp.clip(1.0 + 0.1 * jax.random.normal(splits[1], (LAYERS, D), jnp.float32), 0.5, 1.5),
        "gate_weight": gaussian(splits[2], (LAYERS, D, INNER), D ** -0.5, 0.125, ((0, 2), (2, 8))),
        "inner_weight": gaussian(splits[3], (LAYERS, D, INNER), D ** -0.5, 0.125, ((0, 2), (2, 8))),
        "state_weight": gaussian(splits[4], (LAYERS, D, 2 * STATE), D ** -0.5, 0.125, ((0, 2),)),
        "step_weight": gaussian(splits[5], (LAYERS, D, HEADS), D ** -0.5, 0.125, ((0, 2), (2, 8))),
        "inner_taps": gaussian(splits[6], (LAYERS, KW + 1, INNER), 0.5, 3.0, ((0, 2), (2, 8)), jnp.float32),
        "state_taps": gaussian(splits[7], (LAYERS, KW + 1, 2 * STATE), 0.5, 3.0, ((0, 2),), jnp.float32),
        "step_bias": jnp.clip(-5.0 + 3.0 * jax.random.uniform(splits[8], (LAYERS, HEADS), jnp.float32) ** block_levels(splits[8], (LAYERS, HEADS), ((0, 2), (1, 8)), -0.2, 0.2), -5.0, -2.0),
        "decay_rate": jnp.clip(jnp.exp(math.log(1.0) - 7.624619 * jax.random.uniform(splits[9], (LAYERS, HEADS), jnp.float32) ** block_levels(splits[9], (LAYERS, HEADS), ((0, 2), (1, 8)), -0.2, 0.2)), 0.00048828125, 1.0),
        "skip_scale": jnp.clip(0.5 + 1.0 * jax.random.uniform(splits[10], (LAYERS, HEADS), jnp.float32) ** block_levels(splits[10], (LAYERS, HEADS), ((0, 2), (1, 8)), -0.2, 0.2), 0.5, 1.5),
        "inner_gain": jnp.clip(1.0 + 0.1 * jax.random.normal(splits[11], (LAYERS, INNER), jnp.float32), 0.5, 1.5),
        "out_weight": gaussian(splits[12], (LAYERS, INNER, D), INNER ** -0.5, 0.078125, ((0, 2), (1, 8))),
    }


EPS = 1e-05

def causal_taps(values, taps):
    width = taps.shape[0] - 1
    length = values.shape[0]
    zeros = jnp.zeros((width - 1, values.shape[1]), values.dtype)
    padded = jnp.concatenate([zeros, values], axis=0).astype(jnp.float32)
    total = jnp.broadcast_to(taps[width][None, :], (length, values.shape[1]))
    for index in range(width):
        total = total + taps[index][None, :] * padded[index:index + length]
    return jax.nn.silu(total).astype(jnp.bfloat16)

def block_terms(inner_block, input_block, output_block, step_block, rate):
    size = step_block.shape[0]
    cumulative = jnp.cumsum(-step_block * rate[None, :], axis=0)
    by_head = cumulative.T
    later = jnp.arange(size)[:, None] >= jnp.arange(size)[None, :]
    decay = jnp.exp(jnp.where(later[None], by_head[:, :, None] - by_head[:, None, :], -jnp.inf))
    scores = jnp.dot(output_block, input_block.T, preferred_element_type=jnp.float32)
    mixing = (scores[None] * decay * step_block.T[:, None, :]).astype(jnp.bfloat16)
    inside = jnp.einsum('hqs,shp->qhp', mixing.astype(jnp.float32), inner_block.astype(jnp.float32))
    weighting = jnp.exp(cumulative[-1:] - cumulative) * step_block
    weighted = (inner_block.astype(jnp.float32) * weighting[:, :, None]).astype(jnp.bfloat16)
    state = jnp.einsum('shp,sn->hpn', weighted.astype(jnp.float32), input_block.astype(jnp.float32))
    return (cumulative, inside, state, jnp.exp(cumulative[-1]))

def state_space(inner_conv, state_conv, step_size, rate, skip):
    length = inner_conv.shape[0]
    count = length // BLOCK
    inner_blocks = inner_conv.reshape(count, BLOCK, HEADS, HEADDIM)
    input_blocks = state_conv[:, :STATE].reshape(count, BLOCK, STATE)
    output_blocks = state_conv[:, STATE:].reshape(count, BLOCK, STATE)
    step_blocks = step_size.reshape(count, BLOCK, HEADS)

    def advance(carried, items):
        inner_block, input_block, output_block, step_block = items
        cumulative, inside, state, decay = block_terms(inner_block, input_block, output_block, step_block, rate)
        across = jnp.exp(cumulative)[:, :, None] * jnp.einsum('qn,hpn->qhp', output_block.astype(jnp.float32), carried, precision=lax.Precision.HIGHEST)
        return (carried * decay[:, None, None] + state, inside + across)
    initial = jnp.zeros((HEADS, HEADDIM, STATE), jnp.float32)
    _, pieces = lax.scan(advance, initial, (inner_blocks, input_blocks, output_blocks, step_blocks))
    mixed = pieces + skip[None, None, :, None] * inner_blocks.astype(jnp.float32)
    return mixed.reshape(length, HEADS * HEADDIM)

def layer(current, prenorm, gate_weight, inner_weight, state_weight, step_weight, inner_taps, state_taps, step_bias, decay_rate, skip_scale, inner_gain, out_weight):
    widened = current.astype(jnp.float32)
    normed_in = (widened * lax.rsqrt(lax.optimization_barrier(jnp.mean(widened * widened, axis=1, keepdims=True)) + EPS) * prenorm).astype(jnp.bfloat16)
    gate_raw = jnp.dot(normed_in, gate_weight, preferred_element_type=jnp.float32).astype(jnp.bfloat16)
    inner_raw = jnp.dot(normed_in, inner_weight, preferred_element_type=jnp.float32).astype(jnp.bfloat16)
    state_raw = jnp.dot(normed_in, state_weight, preferred_element_type=jnp.float32).astype(jnp.bfloat16)
    step_raw = jnp.dot(normed_in, step_weight, preferred_element_type=jnp.float32)
    inner_conv = causal_taps(inner_raw, inner_taps)
    state_conv = causal_taps(state_raw, state_taps)
    step_size = jax.nn.softplus(step_raw + step_bias)
    mixed = state_space(inner_conv, state_conv, step_size, decay_rate, skip_scale)
    gated = mixed * jax.nn.silu(gate_raw.astype(jnp.float32))
    normed = (gated * lax.rsqrt(lax.optimization_barrier(jnp.mean(gated * gated, axis=1, keepdims=True)) + EPS) * inner_gain).astype(jnp.bfloat16)
    summed = jnp.dot(normed, out_weight, preferred_element_type=jnp.float32)
    return (widened + summed).astype(jnp.bfloat16)

def reference(tokens, prenorm_gain, gate_weight, inner_weight, state_weight, step_weight, inner_taps, state_taps, step_bias, decay_rate, skip_scale, inner_gain, out_weight):
    results = []
    for micro in range(MICRO):
        current = tokens[micro]
        per_layer = []
        for depth in range(LAYERS):
            current = layer(current, prenorm_gain[depth], gate_weight[depth], inner_weight[depth], state_weight[depth], step_weight[depth], inner_taps[depth], state_taps[depth], step_bias[depth], decay_rate[depth], skip_scale[depth], inner_gain[depth], out_weight[depth])
            per_layer.append(current)
        results.append(jnp.stack(per_layer))
    return jnp.stack(results, axis=1)
```

```python
import jax
import jax.numpy as jnp
from jax import lax
from jax.experimental import pallas as pl
from jax.experimental.pallas import tpu as pltpu
from jax.sharding import PartitionSpec as P

MESH = pl.DeviceIdType.MESH
F32, BF16 = jnp.float32, jnp.bfloat16
HIGHEST = lax.Precision.HIGHEST
EPS = 1e-05
SECTIONS, SHARE, SEQ = 2, 8, 16
CHIPS = SHARE // 2
MICRO, ROWS, WIDTH, INNER = 2, 128, 2560, 5120
NARROW = WIDTH // SHARE
LOCAL = INNER // SHARE
STATE = 128
HEADS = 10
TAPS = 4
SLAB = 384
OWNED = MICRO * STATE // SEQ
OWNERS = SEQ // MICRO
EDGE = 8
BOTH = MICRO * ROWS


def silu(value):
    return value / (1.0 + jnp.exp(-value))


def dot(a, b, **options):
    return jnp.dot(a, b, preferred_element_type=F32, **options)


def remote(src, dst, send, recv, device):
    return pltpu.make_async_remote_copy(
        src_ref=src, dst_ref=dst, send_sem=send, recv_sem=recv, device_id=device, device_id_type=MESH
    )


def kernel(
    tokens, pre_gain, gate_w, inner_w, state_w, step_w, inner_taps, state_taps, step_bias, decay_rate,
    skip_scale, inner_gain, out_w, out,
    x, xg, gains, wi, ws, wd, wg, wo, acc_i, acc_s, acc_d, acc_g, squares, padded, inner_conv, state_conv,
    steps, growth, mixed, decay, decays, sent, arrived, back, entering, normed, halves, partner_half, joined, totals,
    own, local_sem, gather_s, gather_r, rim_s, rim_r, decay_s, decay_r, state_s, state_r, enter_s, enter_r,
    half_s, half_r, total_s, total_r, pipe_s, pipe_r, out_sem,
):
    section, member, place = (lax.axis_index(name) for name in ("pipe", "tensor", "seq"))
    chip, core = member // 2, member % 2
    partner = member + 1 - 2 * core

    loads = [
        pltpu.make_async_copy(source.at[0], target, local_sem.at[index])
        for index, (source, target) in enumerate(
            ((inner_w, wi), (state_w, ws), (step_w, wd), (gate_w, wg), (out_w, wo))
        )
    ]
    fetch = pltpu.make_async_copy(tokens, x.at[member], local_sem.at[5])

    @pl.when(section == 0)
    def _():
        fetch.start()

    for load in loads:
        load.start()

    barrier = pltpu.get_barrier_semaphore()
    pl.semaphore_signal(barrier, inc=1, device_id={"tensor": partner}, device_id_type=MESH)
    pl.semaphore_signal(barrier, inc=1, device_id={"pipe": 1 - section}, device_id_type=MESH)
    for step in range(1, CHIPS):
        other = ((chip + step) % CHIPS) * 2 + core
        pl.semaphore_signal(barrier, inc=1, device_id={"tensor": other}, device_id_type=MESH)
    for step in range(1, SEQ):
        pl.semaphore_signal(barrier, inc=1, device_id={"seq": (place + step) % SEQ}, device_id_type=MESH)

    for k in range(SHARE):
        gains[k] = pre_gain[:, k * NARROW : (k + 1) * NARROW]
    steps[...] = jnp.zeros_like(steps)

    @pl.when(place == 0)
    def _():
        padded[:, 0:EDGE, :] = jnp.zeros((MICRO, EDGE, LOCAL + 2 * STATE), F32)
        entering[...] = jnp.zeros_like(entering)

    pl.semaphore_wait(barrier, 2 + CHIPS - 1 + SEQ - 1)

    handover = remote(own, x.at[member], pipe_s.at[0], pipe_r.at[0], {"pipe": 1})

    @pl.when(section == 0)
    def _():
        fetch.wait()

    @pl.when(section == 1)
    def _():
        handover.wait_recv()

    gathers = []
    for step in (2, 1, 3):
        other = ((chip + step) % CHIPS) * 2 + core
        gathers.append(
            remote(x.at[member], x.at[member], gather_s.at[step], gather_r.at[member], {"tensor": other})
        )
    gathers.append(
        remote(x.at[member], x.at[member], gather_s.at[0], gather_r.at[member], {"tensor": partner})
    )
    for copy in gathers:
        copy.start()
    for load in loads[:3]:
        load.wait()

    def project(index, carry):
        offset = lax.rem(index + 1, 3)
        turn = jnp.where(index < 2, 0, 1 + 2 * offset - 3 * (offset // 2))
        side = jnp.where(jnp.logical_or(index == 1, index > 4), 1 - core, core)
        which = lax.rem(chip + turn, CHIPS) * 2 + side
        block = x.at[which]

        @pl.when(index > 0)
        def _():
            remote(block, block, gather_s.at[0], gather_r.at[which], {"tensor": partner}).wait_recv()

        @pl.when(jnp.logical_and(index > 1, index < 5))
        def _():
            remote(
                block, block, gather_s.at[index + 2], gather_r.at[which], {"tensor": partner}
            ).start()

        wide = x[which].reshape(BOTH, NARROW).astype(F32)
        scaled = (wide * gains[which]).astype(BF16)
        xg[which] = scaled
        depth = pl.ds(pl.multiple_of(which * NARROW, 64), NARROW)
        square = jnp.sum(wide * wide, axis=1, keepdims=True)
        for target, weight in ((acc_i, wi), (acc_s, ws), (acc_d, wd)):
            term = dot(scaled, weight[depth, :])

            @pl.when(index == 0)
            def _():
                target[...] = term

            @pl.when(index > 0)
            def _():
                target[...] += term

        @pl.when(index == 0)
        def _():
            squares[...] = square

        @pl.when(index > 0)
        def _():
            squares[...] += square

        return carry

    lax.fori_loop(0, SHARE, project, 0)

    scale = lax.rsqrt(squares[...] / WIDTH + EPS)
    squares[...] = scale
    for micro in range(MICRO):
        part = slice(micro * ROWS, (micro + 1) * ROWS)
        padded[micro, EDGE : EDGE + ROWS, 0:LOCAL] = (acc_i[part, :] * scale[part]).astype(BF16).astype(F32)
        padded[micro, EDGE : EDGE + ROWS, LOCAL:] = (acc_s[part, :] * scale[part]).astype(BF16).astype(F32)
    rim = remote(
        padded.at[:, ROWS : ROWS + EDGE, :], padded.at[:, 0:EDGE, :], rim_s.at[0], rim_r.at[0],
        {"seq": lax.rem(place + 1, SEQ)},
    )

    @pl.when(place < SEQ - 1)
    def _():
        rim.start()

    shifted = acc_d[...] * scale + step_bias[...]
    steps[:, 0:HEADS] = jnp.maximum(shifted, 0.0) + jnp.log1p(jnp.exp(-jnp.abs(shifted)))

    loads[3].wait()

    def gate(index, carry):
        depth = pl.ds(pl.multiple_of(index * NARROW, 64), NARROW)
        term = dot(xg[index], wg[depth, :])

        @pl.when(index == 0)
        def _():
            acc_g[...] = term

        @pl.when(index > 0)
        def _():
            acc_g[...] += term

        return carry

    lax.fori_loop(0, SHARE, gate, 0)

    row = lax.broadcasted_iota(jnp.int32, (ROWS, ROWS), 0)
    lane = lax.broadcasted_iota(jnp.int32, (ROWS, ROWS), 1)
    first = lane < 64
    later = row >= lane

    @pl.when(place > 0)
    def _():
        rim.wait_recv()

    def send_states(owner):
        remote(
            decay.at[owner // OWNERS], decays.at[place], decay_s.at[owner], decay_r.at[place], {"seq": owner}
        ).start()
        remote(
            sent.at[owner], arrived.at[place], state_s.at[owner], state_r.at[place], {"seq": owner}
        ).start()

    for micro in range(MICRO):
        for column in range(0, LOCAL + 2 * STATE, 128):
            taps, at = (inner_taps, column) if column < LOCAL else (state_taps, column - LOCAL)
            total = jnp.broadcast_to(taps[0, TAPS : TAPS + 1, at : at + 128], (ROWS, 128))
            for index in range(TAPS):
                begin = EDGE - TAPS + 1 + index
                total = total + taps[0, index : index + 1, at : at + 128] * (
                    padded[micro, begin : begin + ROWS, column : column + 128]
                )
            result = silu(total).astype(BF16)
            if column < LOCAL:
                inner_conv[micro, :, at : at + 128] = result
            else:
                state_conv[micro, :, at : at + 128] = result

        part = slice(micro * ROWS, (micro + 1) * ROWS)
        rates = jnp.zeros((1, 128), F32)
        step_size = steps[part, :]
        rates = decays_row(decay_rate)
        cumulative = dot(later.astype(F32), -step_size * rates, precision=HIGHEST)
        across_step, across_sum = step_size.T, cumulative.T
        to_state = state_conv[micro, :, 0:STATE]
        from_state = state_conv[micro, :, STATE:]
        turned = to_state.astype(F32).T.astype(BF16)
        for pair in range(HEADS // 2):
            heads = (2 * pair, 2 * pair + 1)
            at = slice(pair * 128, pair * 128 + 128)
            sums = [jnp.broadcast_to(cumulative[:, h : h + 1], (ROWS, 128)) for h in heads]
            sizes = [jnp.broadcast_to(step_size[:, h : h + 1], (ROWS, 128)) for h in heads]
            each = jnp.where(first, sums[0], sums[1])
            values = inner_conv[micro, :, at].astype(F32)
            weighting = jnp.exp(each[ROWS - 1 :, :] - each) * jnp.where(first, sizes[0], sizes[1])
            state = dot(turned, (values * weighting).astype(BF16)).astype(BF16)
            sent[micro * OWNERS : (micro + 1) * OWNERS, :, at] = state.reshape(OWNERS, OWNED, 128)
            grown = jnp.exp(each)
            growth[micro, :, at] = grown
            decay[micro, :, at] = grown[ROWS - 1 :, :]

        for owner in range(micro * OWNERS, (micro + 1) * OWNERS):

            @pl.when(jnp.logical_and(place != owner, place < SEQ - 1))
            def _():
                send_states(owner)

        scores = lax.dot_general(
            from_state, to_state, (((1,), (1,)), ((), ())), preferred_element_type=F32
        )
        for pair in range(HEADS // 2):
            at = slice(pair * 128, pair * 128 + 128)
            values = inner_conv[micro, :, at]
            parts = []
            for h in (2 * pair, 2 * pair + 1):
                column = jnp.broadcast_to(cumulative[:, h : h + 1], (ROWS, 128))
                fade = jnp.exp(jnp.where(later, column - across_sum[h : h + 1, :], -jnp.inf))
                mixing = (scores * fade * across_step[h : h + 1, :]).astype(BF16)
                parts.append(dot(mixing, values))
            skip = jnp.where(first[0:1], skip_scale[0, 2 * pair], skip_scale[0, 2 * pair + 1])
            mixed[micro, :, at] = jnp.where(first, parts[0], parts[1]) + skip * values.astype(F32)

    arrived[place] = sent[place]
    decays[place] = decay[place // OWNERS]
    carried = jnp.zeros((OWNED, LOCAL), F32)
    for source in range(SEQ):
        if source > 0:
            back[source] = carried.astype(BF16)

            @pl.when(place != source)
            def _():
                remote(
                    back.at[source], entering.at[place], enter_s.at[source], enter_r.at[place],
                    {"seq": source},
                ).start()

        if source < SEQ - 1:

            @pl.when(place != source)
            def _():
                remote(
                    sent.at[source], arrived.at[source], state_s.at[source], state_r.at[source],
                    {"seq": source},
                ).wait_recv()
                remote(
                    decay.at[0], decays.at[source], decay_s.at[source], decay_r.at[source], {"seq": source}
                ).wait_recv()

            carried = decays[source] * carried + arrived[source].astype(F32)

    @pl.when(place > 0)
    def _():
        entering[place] = back[place]

    for micro in range(MICRO):
        for owner in range(micro * OWNERS, (micro + 1) * OWNERS):

            @pl.when(jnp.logical_and(place != owner, place > 0))
            def _():
                remote(
                    back.at[owner], entering.at[owner], enter_s.at[owner], enter_r.at[owner], {"seq": owner}
                ).wait_recv()

        part = slice(micro * ROWS, (micro + 1) * ROWS)
        from_state = state_conv[micro, :, STATE:]
        scale = squares[part, :]
        square = jnp.zeros((ROWS, 1), F32)
        for column in range(0, LOCAL, 128):
            at = slice(column, column + 128)
            entry = entering[micro * OWNERS : (micro + 1) * OWNERS, :, at].reshape(STATE, 128)
            value = mixed[micro, :, at] + growth[micro, :, at] * dot(from_state, entry)
            raw = (acc_g[part, at] * scale).astype(BF16).astype(F32)
            gated = value * silu(raw)
            square = square + jnp.sum(gated * gated, axis=1, keepdims=True)
            normed[part, at] = (gated * inner_gain[:, at]).astype(BF16)
        squares[part, :] = square

    loads[4].wait()
    wide_lane = lax.broadcasted_iota(jnp.int32, (BOTH, SLAB), 1)

    def with_squares(values, total):
        high = total.astype(BF16).astype(F32)
        spare = jnp.where(wide_lane < NARROW + 32, high, total - high)
        return jnp.where(wide_lane < NARROW, values, spare).astype(BF16)

    def to_partner(which):
        return remote(
            halves.at[1 - core, which], partner_half.at[which], half_s.at[which], half_r.at[which],
            {"tensor": partner},
        )

    def to_chip(which):
        return remote(
            joined.at[which], totals.at[chip], total_s.at[which], total_r.at[chip],
            {"tensor": which * 2 + core},
        )

    def spread(index, carry):
        which = lax.rem(chip + 1 + index, CHIPS)
        at = pl.ds(pl.multiple_of(which * 2 * NARROW, 128), 2 * NARROW)
        product = dot(normed[...], wo[:, at])
        turned = pltpu.roll(product, NARROW, 1)
        halves[0, which] = with_squares(product[:, 0:SLAB], squares[...])
        halves[1, which] = with_squares(turned[:, 0:SLAB], squares[...])
        to_partner(which).start()
        return carry

    lax.fori_loop(0, CHIPS, spread, 0)

    def join(index, carry):
        which = lax.rem(chip + 1 + index, CHIPS)
        to_partner(which).wait_recv()
        both = halves[core, which].astype(F32) + partner_half[which].astype(F32)
        total = both[:, NARROW : NARROW + 1] + both[:, NARROW + 32 : NARROW + 33]
        joined[which] = with_squares(both, total)

        @pl.when(index < CHIPS - 1)
        def _():
            to_chip(which).start()

        return carry

    lax.fori_loop(0, CHIPS, join, 0)

    total = joined[chip].astype(F32)
    for step in range(1, CHIPS):
        which = lax.rem(chip + step, CHIPS)
        remote(
            joined.at[which], totals.at[which], total_s.at[which], total_r.at[which],
            {"tensor": which * 2 + core},
        ).wait_recv()
        total = total + totals[which].astype(F32)
    square = total[:, NARROW : NARROW + 1] + total[:, NARROW + 32 : NARROW + 33]
    scale = lax.rsqrt(square / INNER + EPS)
    base = x[member].reshape(BOTH, NARROW).astype(F32)
    own[...] = (base + total[:, 0:NARROW] * scale).astype(BF16).reshape(MICRO, ROWS, NARROW)

    @pl.when(section == 0)
    def _():
        handover.start()

    write = pltpu.make_async_copy(own, out.at[0], out_sem.at[0])
    write.start()

    for copy in gathers:
        copy.wait_send()
    for index in range(2, 5):
        remote(
            x.at[member], x.at[member], gather_s.at[index + 2], gather_r.at[member], {"tensor": partner}
        ).wait_send()

    @pl.when(place < SEQ - 1)
    def _():
        rim.wait_send()

    for owner in range(SEQ):

        @pl.when(jnp.logical_and(place != owner, place < SEQ - 1))
        def _():
            remote(
                decay.at[0], decays.at[owner], decay_s.at[owner], decay_r.at[owner], {"seq": owner}
            ).wait_send()
            remote(
                sent.at[owner], arrived.at[owner], state_s.at[owner], state_r.at[owner], {"seq": owner}
            ).wait_send()

        if owner > 0:

            @pl.when(place != owner)
            def _():
                remote(
                    back.at[owner], entering.at[owner], enter_s.at[owner], enter_r.at[owner], {"seq": owner}
                ).wait_send()

    for step in range(CHIPS):
        which = lax.rem(chip + step, CHIPS)
        to_partner(which).wait_send()
        if step > 0:
            to_chip(which).wait_send()

    @pl.when(section == 0)
    def _():
        handover.wait_send()

    write.wait()


def decays_row(rate):
    return jnp.concatenate([rate[...], jnp.zeros((1, 128 - HEADS), F32)], axis=1)


def shards(*arrays):
    vmem, hbm, smem = (pl.BlockSpec(memory_space=space) for space in (pltpu.VMEM, pl.ANY, pltpu.SMEM))
    dma = lambda count: pltpu.SemaphoreType.DMA((count,))
    return pl.pallas_call(
        kernel,
        out_shape=jax.ShapeDtypeStruct((1, MICRO, ROWS, NARROW), BF16),
        in_specs=[hbm, vmem, hbm, hbm, hbm, hbm, vmem, vmem, vmem, vmem, smem, vmem, hbm],
        out_specs=hbm,
        scratch_shapes=[
            pltpu.VMEM((SHARE, MICRO, ROWS, NARROW), BF16),
            pltpu.VMEM((SHARE, BOTH, NARROW), BF16),
            pltpu.VMEM((SHARE, 1, NARROW), F32),
            pltpu.VMEM((WIDTH, LOCAL), BF16),
            pltpu.VMEM((WIDTH, 2 * STATE), BF16),
            pltpu.VMEM((WIDTH, HEADS), BF16),
            pltpu.VMEM((WIDTH, LOCAL), BF16),
            pltpu.VMEM((LOCAL, WIDTH), BF16),
            pltpu.VMEM((BOTH, LOCAL), F32),
            pltpu.VMEM((BOTH, 2 * STATE), F32),
            pltpu.VMEM((BOTH, HEADS), F32),
            pltpu.VMEM((BOTH, LOCAL), F32),
            pltpu.VMEM((BOTH, 1), F32),
            pltpu.VMEM((MICRO, EDGE + ROWS, LOCAL + 2 * STATE), F32),
            pltpu.VMEM((MICRO, ROWS, LOCAL), BF16),
            pltpu.VMEM((MICRO, ROWS, 2 * STATE), BF16),
            pltpu.VMEM((BOTH, 128), F32),
            pltpu.VMEM((MICRO, ROWS, LOCAL), F32),
            pltpu.VMEM((MICRO, ROWS, LOCAL), F32),
            pltpu.VMEM((MICRO, 1, LOCAL), F32),
            pltpu.VMEM((SEQ, 1, LOCAL), F32),
            pltpu.VMEM((SEQ, OWNED, LOCAL), BF16),
            pltpu.VMEM((SEQ, OWNED, LOCAL), BF16),
            pltpu.VMEM((SEQ, OWNED, LOCAL), BF16),
            pltpu.VMEM((SEQ, OWNED, LOCAL), BF16),
            pltpu.VMEM((BOTH, LOCAL), BF16),
            pltpu.VMEM((2, CHIPS, BOTH, SLAB), BF16),
            pltpu.VMEM((CHIPS, BOTH, SLAB), BF16),
            pltpu.VMEM((CHIPS, BOTH, SLAB), BF16),
            pltpu.VMEM((CHIPS, BOTH, SLAB), BF16),
            pltpu.VMEM((MICRO, ROWS, NARROW), BF16),
            dma(6), dma(7), dma(SHARE), dma(1), dma(1), dma(SEQ), dma(SEQ), dma(SEQ), dma(SEQ), dma(SEQ), dma(SEQ),
            dma(CHIPS), dma(CHIPS), dma(CHIPS), dma(CHIPS), dma(1), dma(1), dma(1),
        ],
        compiler_params=pltpu.CompilerParams(
            collective_id=0, has_side_effects=True, vmem_limit_bytes=48 * 1024 * 1024
        ),
    )(*arrays)


def solution(mesh):
    return jax.shard_map(
        shards,
        mesh=mesh,
        in_specs=(
            P(None, "seq", "tensor"),
            P("pipe", None),
            P("pipe", None, "tensor"),
            P("pipe", None, "tensor"),
            P("pipe", None, None),
            P("pipe", None, "tensor"),
            P("pipe", None, "tensor"),
            P("pipe", None, None),
            P("pipe", "tensor"),
            P("pipe", "tensor"),
            P("pipe", "tensor"),
            P("pipe", "tensor"),
            P("pipe", "tensor", None),
        ),
        out_specs=P("pipe", None, "seq", "tensor"),
        check_vma=False,
    )
```

```python
import jax
import jax.numpy as jnp
from jax import lax
from jax.experimental import pallas as pl
from jax.experimental.pallas import tpu as pltpu
from jax.sharding import PartitionSpec as P

MESH = pl.DeviceIdType.MESH
F32, BF16 = jnp.float32, jnp.bfloat16
HIGHEST = lax.Precision.HIGHEST
EPS = 1e-05
SHARE, SEQ = 8, 16
CHIPS = SHARE // 2
MICRO, ROWS, WIDTH, INNER = 2, 128, 2560, 5120
NARROW = WIDTH // SHARE
PAIR = 2 * NARROW
LOCAL = INNER // SHARE
STATE = 128
BOTH = LOCAL + 2 * STATE
HEADS = 10
TAPS = 4
SLAB = NARROW + 16
OWNED = MICRO * STATE // SEQ
OWNERS = SEQ // MICRO
EDGE = 8
SENDS = 7


def silu(value):
    return value / (1.0 + jnp.exp(-value))


def dot(a, b, **options):
    return jnp.dot(a, b, preferred_element_type=F32, **options)


def dot_turned(a, b):
    return lax.dot_general(a, b, (((1,), (1,)), ((), ())), preferred_element_type=F32)


def remote(src, dst, send, recv, device):
    return pltpu.make_async_remote_copy(
        src_ref=src, dst_ref=dst, send_sem=send, recv_sem=recv, device_id=device, device_id_type=MESH
    )


def kernel(
    tokens, pre_gain_h, gate_h, inner_h, state_h, step_h, inner_taps_h, state_taps_h, bias_h, rate_h, skip_h, gain_h,
    out_h, out,
    x, xg, w1, wd, wg, wo, pre_gain, inner_taps, state_taps, bias, rate, skip_scale, inner_gain,
    acc, acc_d, gate_act, squares, scales, padded, inner_conv, state_conv, steps, sums, growth, mixed, decay, decays, sent,
    arrived, back, entering, normed, halves, partner_half, joined, before, totals, own, relay,
    local_s, gather_s, gather_r, rim_s, rim_r, decay_s, decay_r, state_s, state_r, enter_s, enter_r, half_s, half_r,
    before_s, before_r, total_s, total_r, pipe_s, pipe_r, pass_s, pass_r, out_s,
):
    section, member, place = (lax.axis_index(name) for name in ("pipe", "tensor", "seq"))
    chip, core = member // 2, member % 2
    partner = member + 1 - 2 * core
    beside = place + 1 - 2 * lax.rem(place, 2)
    after, behind, across_ring = (lax.rem(chip + step, CHIPS) for step in (1, CHIPS - 1, 2))

    def device(which):
        return {"tensor": which * 2 + core}

    loads = [
        pltpu.make_async_copy(source, target, local_s.at[index])
        for index, (source, target) in enumerate(
            (
                (tokens.at[0], x.at[chip, 0, core]),
                (tokens.at[1], x.at[chip, 1, core]),
                (inner_h.at[0], w1.at[:, 0:LOCAL]),
                (state_h.at[0], w1.at[:, LOCAL:BOTH]),
                (step_h.at[0], wd),
                (pre_gain_h, pre_gain),
                (inner_taps_h, inner_taps),
                (state_taps_h, state_taps),
                (bias_h, bias),
                (rate_h, rate),
                (skip_h, skip_scale),
                (gain_h, inner_gain),
                (gate_h.at[0], wg),
                (out_h.at[0], wo),
            )
        )
    ]

    @pl.when(section == 0)
    def _():
        for load in loads[:MICRO]:
            load.start()

    for load in loads[MICRO:]:
        load.start()

    barrier = pltpu.get_barrier_semaphore()

    def greet(peer):
        pl.semaphore_signal(barrier, inc=1, device_id=peer, device_id_type=MESH)

    for step in range(1, SEQ):
        greet({"seq": lax.rem(place + step, SEQ)})
    greet({"pipe": 1 - section, "seq": beside})
    greet(device(after))
    greet(device(behind))
    greet({"tensor": partner})

    steps[...] = jnp.zeros_like(steps)

    @pl.when(place == 0)
    def _():
        padded[:, 0:EDGE, :] = jnp.zeros((MICRO, EDGE, BOTH), F32)
        entering[...] = jnp.zeros_like(entering)

    pl.semaphore_wait(barrier, SEQ - 1 + 4)

    def handover(micro):
        return remote(
            own.at[micro], relay.at[micro], pipe_s.at[micro], pipe_r.at[micro], {"pipe": 1, "seq": beside}
        )

    def passing(micro):
        return remote(
            relay.at[micro], x.at[chip, micro, core], pass_s.at[micro], pass_r.at[micro], {"seq": beside}
        )

    def slab(which, side, micro, target, send):
        block = x.at[which, micro, side]
        return remote(
            block, block, gather_s.at[micro * SENDS + send], gather_r.at[(which * 2 + side) * MICRO + micro], target
        )

    to_partner = {"tensor": partner}

    def gather(micro, send):
        onward, backward = (behind, after) if micro == 0 else (after, behind)
        which, side, target = (
            (chip, core, device(after)),
            (chip, core, device(behind)),
            (chip, core, to_partner),
            (onward, core, device(backward)),
            (onward, core, to_partner),
            (backward, core, to_partner),
            (across_ring, core, to_partner),
        )[send]
        return slab(which, side, micro, target, send)

    def send_own(micro):
        @pl.when(section == 0)
        def _():
            loads[micro].wait()

        @pl.when(section == 1)
        def _():
            handover(micro).wait_recv()
            passing(micro).start()
            passing(micro).wait_recv()

        for send in range(3):
            gather(micro, send).start()

    def forward_near(micro):
        gather(micro, 4).wait_recv()
        gather(micro, 3).start()
        gather(micro, 4).start()
        gather(micro, 5).wait_recv()
        gather(micro, 5).start()

    def forward_far(micro):
        copy = gather(micro, 6)
        copy.wait_recv()
        copy.start()

    def project(micro, which, first):
        slab(which, 1 - core, micro, to_partner, 0).wait_recv()
        wide = x[which, micro].reshape(PAIR, ROWS).astype(F32).T
        at = pl.ds(pl.multiple_of(which * PAIR, 128), PAIR)
        scaled = (wide * pre_gain[:, at]).astype(BF16)
        xg[micro, :, at] = scaled
        square = wide * wide
        square = sum(square[:, column : column + 128] for column in range(0, PAIR, 128))
        term = dot(scaled, w1[at, :])
        term_d = dot_turned(scaled, wd[:, at])
        if first:
            acc[micro], acc_d[micro], squares[micro] = term, term_d, square
        else:
            acc[micro] += term
            acc_d[micro] += term_d
            squares[micro] += square

    def rim(micro):
        return remote(
            padded.at[micro, ROWS : ROWS + EDGE, :], padded.at[micro, 0:EDGE, :], rim_s.at[micro], rim_r.at[micro],
            {"seq": lax.rem(place + 1, SEQ)},
        )

    def project_end(micro):
        scale = lax.rsqrt(jnp.sum(squares[micro], axis=1, keepdims=True) / WIDTH + EPS)
        scales[micro] = scale
        padded[micro, EDGE : EDGE + ROWS, :] = (acc[micro] * scale).astype(BF16).astype(F32)

        @pl.when(place < SEQ - 1)
        def _():
            rim(micro).start()

        shifted = acc_d[micro] * scale + bias[...]
        steps[micro, :, 0:HEADS] = jnp.maximum(shifted, 0.0) + jnp.log1p(jnp.exp(-jnp.abs(shifted)))

    row = lax.broadcasted_iota(jnp.int32, (ROWS, ROWS), 0)
    lane = lax.broadcasted_iota(jnp.int32, (ROWS, ROWS), 1)
    first_half = lane < 64
    later = row >= lane

    def states(micro):
        rates = jnp.concatenate([rate[...], jnp.zeros((1, 128 - HEADS), F32)], axis=1)
        step_size = steps[micro]
        cumulative = dot(later.astype(F32), -step_size * rates, precision=HIGHEST)
        sums[micro] = cumulative

        @pl.when(place > 0)
        def _():
            rim(micro).wait_recv()

        for column in range(0, BOTH, 128):
            taps, at = (inner_taps, column) if column < LOCAL else (state_taps, column - LOCAL)
            total = jnp.broadcast_to(taps[TAPS, :, at : at + 128], (ROWS, 128))
            for index in range(TAPS):
                begin = EDGE - TAPS + 1 + index
                total = total + taps[index, :, at : at + 128] * (
                    padded[micro, begin : begin + ROWS, column : column + 128]
                )
            result = silu(total).astype(BF16)
            if column < LOCAL:
                inner_conv[micro, :, at : at + 128] = result
            else:
                state_conv[micro, :, at : at + 128] = result

        turned = state_conv[micro, :, 0:STATE].astype(F32).T.astype(BF16)
        for pair in range(HEADS // 2):
            heads = (2 * pair, 2 * pair + 1)
            at = slice(pair * 128, pair * 128 + 128)
            spread = [jnp.broadcast_to(cumulative[:, h : h + 1], (ROWS, 128)) for h in heads]
            sizes = [jnp.broadcast_to(step_size[:, h : h + 1], (ROWS, 128)) for h in heads]
            each = jnp.where(first_half, spread[0], spread[1])
            values = inner_conv[micro, :, at].astype(F32)
            weighting = jnp.exp(each[ROWS - 1 :, :] - each) * jnp.where(first_half, sizes[0], sizes[1])
            state = dot(turned, (values * weighting).astype(BF16)).astype(BF16)
            sent[micro * OWNERS : (micro + 1) * OWNERS, :, at] = state.reshape(OWNERS, OWNED, 128)
            grown = jnp.exp(each)
            growth[micro, :, at] = grown
            decay[micro, :, at] = grown[ROWS - 1 :, :]

    def decay_to(owner):
        return remote(
            decay.at[owner // OWNERS], decays.at[place], decay_s.at[owner], decay_r.at[place], {"seq": owner}
        )

    def state_to(owner):
        return remote(sent.at[owner], arrived.at[place], state_s.at[owner], state_r.at[place], {"seq": owner})

    def enter_to(owner):
        return remote(back.at[owner], entering.at[place], enter_s.at[owner], enter_r.at[place], {"seq": owner})

    def send_states(micro):
        for owner in range(micro * OWNERS, (micro + 1) * OWNERS):

            @pl.when(jnp.logical_and(place != owner, place < SEQ - 1))
            def _():
                decay_to(owner).start()
                state_to(owner).start()

    def gate(micro):
        raw = (dot(xg[micro], wg[...]) * scales[micro]).astype(BF16).astype(F32)
        gate_act[micro] = silu(raw)

    def inside(micro):
        cumulative, step_size = sums[micro], steps[micro]
        across_step, across_sum = step_size.T, cumulative.T
        scores = dot_turned(state_conv[micro, :, STATE:], state_conv[micro, :, 0:STATE])
        for pair in range(HEADS // 2):
            at = slice(pair * 128, pair * 128 + 128)
            values = inner_conv[micro, :, at]
            parts = []
            for h in (2 * pair, 2 * pair + 1):
                column = jnp.broadcast_to(cumulative[:, h : h + 1], (ROWS, 128))
                fade = jnp.exp(jnp.where(later, column - across_sum[h : h + 1, :], -jnp.inf))
                mixing = (scores * fade * across_step[h : h + 1, :]).astype(BF16)
                parts.append(dot(mixing, values))
            skips = [jnp.broadcast_to(skip_scale[:, h : h + 1], (1, 128)) for h in (2 * pair, 2 * pair + 1)]
            skip = jnp.where(first_half[0:1], skips[0], skips[1])
            mixed[micro, :, at] = jnp.where(first_half, parts[0], parts[1]) + skip * values.astype(F32)

    def scan():
        arrived[place] = sent[place]
        decays[place] = decay[place // OWNERS]
        carried = jnp.zeros((OWNED, LOCAL), F32)
        for source in range(SEQ):
            if source > 0:
                back[source] = carried.astype(BF16)

                @pl.when(place != source)
                def _():
                    enter_to(source).start()

            if source < SEQ - 1:

                @pl.when(place != source)
                def _():
                    remote(
                        sent.at[source], arrived.at[source], state_s.at[source], state_r.at[source], {"seq": source}
                    ).wait_recv()
                    remote(
                        decay.at[0], decays.at[source], decay_s.at[source], decay_r.at[source], {"seq": source}
                    ).wait_recv()

                carried = decays[source] * carried + arrived[source].astype(F32)

        @pl.when(place > 0)
        def _():
            entering[place] = back[place]

    def across(micro):
        for owner in range(micro * OWNERS, (micro + 1) * OWNERS):

            @pl.when(jnp.logical_and(place != owner, place > 0))
            def _():
                remote(
                    back.at[owner], entering.at[owner], enter_s.at[owner], enter_r.at[owner], {"seq": owner}
                ).wait_recv()

        from_state = state_conv[micro, :, STATE:]
        square = jnp.zeros((ROWS, 128), F32)
        for column in range(0, LOCAL, 128):
            at = slice(column, column + 128)
            entry = entering[micro * OWNERS : (micro + 1) * OWNERS, :, at].reshape(STATE, 128)
            value = mixed[micro, :, at] + growth[micro, :, at] * dot(from_state, entry)
            gated = value * gate_act[micro, :, at]
            square = square + gated * gated
            normed[micro, :, at] = (gated * inner_gain[:, at]).astype(BF16)
        return jnp.sum(square.T, axis=0, keepdims=True)

    spare_row = lax.broadcasted_iota(jnp.int32, (16, ROWS), 0)

    def split(total):
        high = total.astype(BF16).astype(F32)
        return jnp.where(spare_row < 8, high, total - high).astype(BF16)

    def half(micro, which):
        index = micro * CHIPS + which
        return remote(
            halves.at[micro, which, 1 - core], partner_half.at[micro, which], half_s.at[index], half_r.at[index],
            to_partner,
        )

    def spread(micro, total, which):
        at = pl.ds(pl.multiple_of(which * PAIR, 128), PAIR)
        product = dot(normed[micro], wo[:, at]).T
        spare = split(total)
        for side in range(2):
            halves[micro, which, side, 0:NARROW, :] = product[side * NARROW : (side + 1) * NARROW, :].astype(BF16)
            halves[micro, which, side, NARROW:SLAB, :] = spare
        half(micro, which).start()

    def unpacked(block):
        wide = block.astype(F32)
        return wide[0:NARROW], wide[NARROW : NARROW + 1] + wide[NARROW + 8 : NARROW + 9]

    def added(*terms):
        return tuple(sum(parts[1:], parts[0]) for parts in zip(*terms))

    def join(micro, which):
        half(micro, which).wait_recv()
        return added(unpacked(halves[micro, which, core]), unpacked(partner_half[micro, which]))

    def pack(micro, which, value):
        joined[micro, which, 0:NARROW, :] = value[0].astype(BF16)
        joined[micro, which, NARROW:SLAB, :] = split(value[1])

    def ways(micro):
        return (after, behind) if micro == 0 else (behind, after)

    def send_before(micro):
        through, _ = ways(micro)
        return remote(
            joined.at[micro, across_ring], before.at[micro], before_s.at[micro], before_r.at[micro], device(through)
        )

    def send_total(micro, way):
        which = ways(micro)[1 - way]
        index = micro * 2 + way
        return remote(
            joined.at[micro, which], totals.at[micro, way], total_s.at[index], total_r.at[index], device(which)
        )

    def spread_all(micro, total):
        through, direct = ways(micro)
        for which in (across_ring, direct, through, chip):
            spread(micro, total, which)

    def join_first(micro):
        _, direct = ways(micro)
        pack(micro, across_ring, join(micro, across_ring))
        send_before(micro).start()
        pack(micro, direct, join(micro, direct))
        send_total(micro, 0).start()

    def join_second(micro):
        through, _ = ways(micro)
        value = join(micro, through)
        send_before(micro).wait_recv()
        pack(micro, through, added(value, unpacked(before[micro])))
        send_total(micro, 1).start()

    def write(micro):
        return pltpu.make_async_copy(own.at[micro], out.at[0, micro], out_s.at[micro])

    def finish(micro):
        value = join(micro, chip)
        for way in range(2):
            send_total(micro, way).wait_recv()
            value = added(value, unpacked(totals[micro, way]))
        base = x[chip, micro, core].astype(F32)
        own[micro] = (base + value[0] * lax.rsqrt(value[1] / INNER + EPS)).astype(BF16)

        @pl.when(section == 0)
        def _():
            handover(micro).start()

        write(micro).start()

    scope = jax.named_scope
    with scope("own"):
        send_own(0)
        send_own(1)
    for load in loads[MICRO:12]:
        load.wait()
    with scope("near"):
        forward_near(0)
        project(0, chip, True)
        forward_near(1)
        project(1, chip, True)
    with scope("project"):
        project(0, after, False)
        project(0, behind, False)
        forward_far(0)
        project(1, after, False)
        project(1, behind, False)
        project(0, across_ring, False)
        project_end(0)
        forward_far(1)
        project(1, across_ring, False)
        project_end(1)
    with scope("states"):
        for micro in range(MICRO):
            states(micro)
            send_states(micro)
    with scope("fill"):
        for load in loads[12:]:
            load.wait()
        for micro in range(MICRO):
            gate(micro)
            inside(micro)
    with scope("scan"):
        scan()
    with scope("across0"):
        total = across(0)
    with scope("spread0"):
        spread_all(0, total)
    with scope("join0"):
        join_first(0)
    with scope("across1"):
        total = across(1)
    with scope("spread1"):
        spread_all(1, total)
    with scope("join1"):
        join_first(1)
    with scope("second"):
        join_second(0)
        join_second(1)
    with scope("finish"):
        finish(0)
        finish(1)

    for micro in range(MICRO):
        for send in range(SENDS):
            gather(micro, send).wait_send()
        for which in (across_ring, after, behind, chip):
            half(micro, which).wait_send()
        send_before(micro).wait_send()
        for way in range(2):
            send_total(micro, way).wait_send()

        @pl.when(place < SEQ - 1)
        def _():
            rim(micro).wait_send()

        @pl.when(section == 0)
        def _():
            handover(micro).wait_send()

        @pl.when(section == 1)
        def _():
            passing(micro).wait_send()

        write(micro).wait()

    for owner in range(SEQ):

        @pl.when(jnp.logical_and(place != owner, place < SEQ - 1))
        def _():
            decay_to(owner).wait_send()
            state_to(owner).wait_send()

        if owner > 0:

            @pl.when(place != owner)
            def _():
                enter_to(owner).wait_send()


def shards(
    tokens, pre_gain, gate_w, inner_w, state_w, step_w, inner_taps, state_taps, step_bias, decay_rate, skip_scale,
    inner_gain, out_w,
):
    hbm = pl.BlockSpec(memory_space=pltpu.HBM)
    dma = lambda count: pltpu.SemaphoreType.DMA((count,))
    result = pl.pallas_call(
        kernel,
        out_shape=jax.ShapeDtypeStruct((1, MICRO, NARROW, ROWS), BF16),
        in_specs=[hbm] * 13,
        out_specs=hbm,
        scratch_shapes=[
            pltpu.VMEM((CHIPS, MICRO, 2, NARROW, ROWS), BF16),
            pltpu.VMEM((MICRO, ROWS, WIDTH), BF16),
            pltpu.VMEM((WIDTH, BOTH), BF16),
            pltpu.VMEM((HEADS, WIDTH), BF16),
            pltpu.VMEM((WIDTH, LOCAL), BF16),
            pltpu.VMEM((LOCAL, WIDTH), BF16),
            pltpu.VMEM((1, WIDTH), F32),
            pltpu.VMEM((TAPS + 1, 1, LOCAL), F32),
            pltpu.VMEM((TAPS + 1, 1, 2 * STATE), F32),
            pltpu.VMEM((1, HEADS), F32),
            pltpu.VMEM((1, HEADS), F32),
            pltpu.VMEM((1, HEADS), F32),
            pltpu.VMEM((1, LOCAL), F32),
            pltpu.VMEM((MICRO, ROWS, BOTH), F32),
            pltpu.VMEM((MICRO, ROWS, HEADS), F32),
            pltpu.VMEM((MICRO, ROWS, LOCAL), F32),
            pltpu.VMEM((MICRO, ROWS, 128), F32),
            pltpu.VMEM((MICRO, ROWS, 1), F32),
            pltpu.VMEM((MICRO, EDGE + ROWS, BOTH), F32),
            pltpu.VMEM((MICRO, ROWS, LOCAL), BF16),
            pltpu.VMEM((MICRO, ROWS, 2 * STATE), BF16),
            pltpu.VMEM((MICRO, ROWS, 128), F32),
            pltpu.VMEM((MICRO, ROWS, 128), F32),
            pltpu.VMEM((MICRO, ROWS, LOCAL), F32),
            pltpu.VMEM((MICRO, ROWS, LOCAL), F32),
            pltpu.VMEM((MICRO, 1, LOCAL), F32),
            pltpu.VMEM((SEQ, 1, LOCAL), F32),
            pltpu.VMEM((SEQ, OWNED, LOCAL), BF16),
            pltpu.VMEM((SEQ, OWNED, LOCAL), BF16),
            pltpu.VMEM((SEQ, OWNED, LOCAL), BF16),
            pltpu.VMEM((SEQ, OWNED, LOCAL), BF16),
            pltpu.VMEM((MICRO, ROWS, LOCAL), BF16),
            pltpu.VMEM((MICRO, CHIPS, 2, SLAB, ROWS), BF16),
            pltpu.VMEM((MICRO, CHIPS, SLAB, ROWS), BF16),
            pltpu.VMEM((MICRO, CHIPS, SLAB, ROWS), BF16),
            pltpu.VMEM((MICRO, SLAB, ROWS), BF16),
            pltpu.VMEM((MICRO, 2, SLAB, ROWS), BF16),
            pltpu.VMEM((MICRO, NARROW, ROWS), BF16),
            pltpu.VMEM((MICRO, NARROW, ROWS), BF16),
            dma(14), dma(MICRO * SENDS), dma(SHARE * MICRO), dma(MICRO), dma(MICRO),
            dma(SEQ), dma(SEQ), dma(SEQ), dma(SEQ), dma(SEQ), dma(SEQ),
            dma(MICRO * CHIPS), dma(MICRO * CHIPS), dma(MICRO), dma(MICRO), dma(MICRO * 2), dma(MICRO * 2),
            dma(MICRO), dma(MICRO), dma(MICRO), dma(MICRO), dma(MICRO),
        ],
        compiler_params=pltpu.CompilerParams(
            collective_id=0, has_side_effects=True, vmem_limit_bytes=56 * 1024 * 1024
        ),
    )(
        jnp.swapaxes(tokens, 1, 2), pre_gain, gate_w, inner_w, state_w, jnp.swapaxes(step_w, 1, 2),
        jnp.swapaxes(inner_taps, 0, 1), jnp.swapaxes(state_taps, 0, 1), step_bias, decay_rate, skip_scale, inner_gain,
        out_w,
    )
    return jnp.swapaxes(result, 2, 3)


def solution(mesh):
    return jax.shard_map(
        shards,
        mesh=mesh,
        in_specs=(
            P(None, "seq", "tensor"),
            P("pipe", None),
            P("pipe", None, "tensor"),
            P("pipe", None, "tensor"),
            P("pipe", None, None),
            P("pipe", None, "tensor"),
            P("pipe", None, "tensor"),
            P("pipe", None, None),
            P("pipe", "tensor"),
            P("pipe", "tensor"),
            P("pipe", "tensor"),
            P("pipe", "tensor"),
            P("pipe", "tensor", None),
        ),
        out_specs=P("pipe", None, "seq", "tensor"),
        check_vma=False,
    )
```

```python
import jax
import jax.numpy as jnp
from jax import lax
from jax.experimental import pallas as pl
from jax.experimental.pallas import tpu as pltpu
from jax.sharding import PartitionSpec as P

MESH = pl.DeviceIdType.MESH
F32, BF16 = jnp.float32, jnp.bfloat16
HIGHEST = lax.Precision.HIGHEST
EPS = 1e-05
SHARE, SEQ = 8, 16
CHIPS = SHARE // 2
MICRO, ROWS, WIDTH, INNER = 2, 128, 2560, 5120
NARROW = WIDTH // SHARE
PAIR = 2 * NARROW
LOCAL = INNER // SHARE
STATE = 128
BOTH = LOCAL + 2 * STATE
HEADS = 10
TAPS = 4
SLAB = NARROW + 16
OWNED = STATE // SEQ
EDGE = 8
HALF = NARROW // 2
SENDS = 10
EARLY, LATE = slice(0, HALF), slice(HALF, NARROW)
PARTS = (slice(0, HALF), slice(HALF, SLAB))


def silu(value):
    return value / (1.0 + jnp.exp(-value))


def dot(a, b, **options):
    return jnp.dot(a, b, preferred_element_type=F32, **options)


def dot_turned(a, b):
    return lax.dot_general(a, b, (((1,), (1,)), ((), ())), preferred_element_type=F32)


def remote(src, dst, send, recv, device):
    return pltpu.make_async_remote_copy(
        src_ref=src, dst_ref=dst, send_sem=send, recv_sem=recv, device_id=device, device_id_type=MESH
    )


def kernel(
    tokens, pre_gain_h, gate_h, inner_h, state_h, step_h, inner_taps_h, state_taps_h, bias_h, rate_h, skip_h, gain_h,
    out_h, out,
    x, xg, w1, wd, wg, wo, pre_gain, inner_taps, state_taps, bias, rate, skip_scale, inner_gain,
    acc, acc_d, gate_act, squares, scales, padded, inner_conv, state_conv, steps, sums, growth, mixed, decay, decays, sent,
    arrived, back, entering, normed, halves, partner_half, joined, before, totals, own,
    local_s, gather_s, gather_r, share_r, rim_s, rim_r, decay_s, decay_r, state_s, state_r, enter_s, enter_r, half_s, half_r,
    before_s, before_r, total_s, total_r, pipe_s, pipe_r,
):
    section, member, place = (lax.axis_index(name) for name in ("pipe", "tensor", "seq"))
    chip, core = member // 2, member % 2
    partner = member + 1 - 2 * core
    after, behind, across_ring = (lax.rem(chip + step, CHIPS) for step in (1, CHIPS - 1, 2))

    def device(which):
        return {"tensor": which * 2 + core}

    loads = [
        pltpu.make_async_copy(source, target, local_s.at[index])
        for index, (source, target) in enumerate(
            (
                (tokens.at[0], x.at[chip, 0, core]),
                (tokens.at[1], x.at[chip, 1, core]),
                (inner_h.at[0], w1.at[:, 0:LOCAL]),
                (state_h.at[0], w1.at[:, LOCAL:BOTH]),
                (step_h.at[0], wd),
                (pre_gain_h, pre_gain),
                (inner_taps_h, inner_taps),
                (state_taps_h, state_taps),
                (bias_h, bias),
                (rate_h, rate),
                (skip_h, skip_scale),
                (gain_h, inner_gain),
                (gate_h.at[0], wg),
                (out_h.at[0], wo),
            )
        )
    ]

    @pl.when(section == 0)
    def _():
        for load in loads[:MICRO]:
            load.start()

    for load in loads[MICRO:]:
        load.start()

    barrier = pltpu.get_barrier_semaphore()

    def greet(peer):
        pl.semaphore_signal(barrier, inc=1, device_id=peer, device_id_type=MESH)

    for step in range(1, SEQ):
        greet({"seq": lax.rem(place + step, SEQ)})
    greet({"pipe": 1 - section})
    greet(device(after))
    greet(device(behind))
    greet({"tensor": partner})

    steps[...] = jnp.zeros_like(steps)

    @pl.when(place == 0)
    def _():
        padded[:, 0:EDGE, :] = jnp.zeros((MICRO, EDGE, BOTH), F32)
        entering[...] = jnp.zeros_like(entering)

    pl.semaphore_wait(barrier, SEQ - 1 + 4)

    def handover(micro, part):
        index, rows = micro * 2 + part, (EARLY, LATE)[part]
        return remote(
            own.at[micro, rows], x.at[chip, micro, core, rows], pipe_s.at[index], pipe_r.at[index], {"pipe": 1}
        )

    to_partner = {"tensor": partner}

    def gather(micro, send):
        which, part, target = (
            (chip, 0, after),
            (chip, 1, behind),
            (chip, 1, after),
            (chip, 0, behind),
            (behind, 0, after),
            (after, 1, behind),
            (chip, 2, None),
            (behind, 2, None),
            (after, 2, None),
            (across_ring, 2, None),
        )[send]
        send_sem = gather_s.at[micro * SENDS + send]
        if part == 2:
            block = x.at[which, micro, core]
            return remote(block, block, send_sem, share_r.at[which * MICRO + micro], to_partner)
        block = x.at[which, micro, core, (EARLY, LATE)[part]]
        return remote(block, block, send_sem, gather_r.at[(which * MICRO + micro) * 2 + part], device(target))

    def arrival(micro, which, part):
        block = x.at[which, micro, core, (EARLY, LATE)[part]]
        index = (which * MICRO + micro) * 2 + part
        return remote(block, block, gather_s.at[micro * SENDS], gather_r.at[index], to_partner)

    def shared(micro, which):
        block = x.at[which, micro, 1 - core]
        return remote(block, block, gather_s.at[micro * SENDS], share_r.at[which * MICRO + micro], to_partner)

    def start_own(micro):
        for send in (0, 1, 2, 3, 6):
            gather(micro, send).start()

    def send_loaded(micro):
        @pl.when(section == 0)
        def _():
            loads[micro].wait()
            start_own(micro)

    def send_passed(micro):
        @pl.when(section == 1)
        def _():
            for part in range(2):
                handover(micro, part).wait_recv()
            start_own(micro)

    def forward_near(micro):
        arrival(micro, behind, 0).wait_recv()
        gather(micro, 4).start()
        arrival(micro, after, 1).wait_recv()
        gather(micro, 5).start()
        arrival(micro, behind, 1).wait_recv()
        gather(micro, 7).start()
        arrival(micro, after, 0).wait_recv()
        gather(micro, 8).start()

    def forward_far(micro):
        arrival(micro, across_ring, 0).wait_recv()
        arrival(micro, across_ring, 1).wait_recv()
        gather(micro, 9).start()

    def project(micro, which, first):
        shared(micro, which).wait_recv()
        wide = x[which, micro].reshape(PAIR, ROWS).astype(F32).T
        at = pl.ds(pl.multiple_of(which * PAIR, 128), PAIR)
        scaled = (wide * pre_gain[:, at]).astype(BF16)
        xg[micro, :, at] = scaled
        square = wide * wide
        square = sum(square[:, column : column + 128] for column in range(0, PAIR, 128))
        term = dot(scaled, w1[at, :])
        term_d = dot_turned(scaled, wd[:, at])
        if first:
            acc[micro], acc_d[micro], squares[micro] = term, term_d, square
        else:
            acc[micro] += term
            acc_d[micro] += term_d
            squares[micro] += square

    def rim(micro):
        return remote(
            padded.at[micro, ROWS : ROWS + EDGE, :], padded.at[micro, 0:EDGE, :], rim_s.at[micro], rim_r.at[micro],
            {"seq": lax.rem(place + 1, SEQ)},
        )

    def project_end(micro):
        scale = lax.rsqrt(jnp.sum(squares[micro], axis=1, keepdims=True) / WIDTH + EPS)
        scales[micro] = scale
        padded[micro, EDGE : EDGE + ROWS, :] = (acc[micro] * scale).astype(BF16).astype(F32)

        @pl.when(place < SEQ - 1)
        def _():
            rim(micro).start()

        shifted = acc_d[micro] * scale + bias[...]
        steps[micro, :, 0:HEADS] = jnp.maximum(shifted, 0.0) + jnp.log1p(jnp.exp(-jnp.abs(shifted)))

    row = lax.broadcasted_iota(jnp.int32, (ROWS, ROWS), 0)
    lane = lax.broadcasted_iota(jnp.int32, (ROWS, ROWS), 1)
    first_half = lane < 64
    later = row >= lane

    def states(micro):
        rates = jnp.concatenate([rate[...], jnp.zeros((1, 128 - HEADS), F32)], axis=1)
        step_size = steps[micro]
        cumulative = dot(later.astype(F32), -step_size * rates, precision=HIGHEST)
        sums[micro] = cumulative
        decay[micro] = jnp.exp(cumulative[ROWS - 1 :, :])

        @pl.when(place > 0)
        def _():
            rim(micro).wait_recv()

        for column in range(0, BOTH, 128):
            taps, at = (inner_taps, column) if column < LOCAL else (state_taps, column - LOCAL)
            total = jnp.broadcast_to(taps[TAPS, :, at : at + 128], (ROWS, 128))
            for index in range(TAPS):
                begin = EDGE - TAPS + 1 + index
                total = total + taps[index, :, at : at + 128] * (
                    padded[micro, begin : begin + ROWS, column : column + 128]
                )
            result = silu(total).astype(BF16)
            if column < LOCAL:
                inner_conv[micro, :, at : at + 128] = result
            else:
                state_conv[micro, :, at : at + 128] = result

        turned = state_conv[micro, :, 0:STATE].astype(F32).T.astype(BF16)
        for pair in range(HEADS // 2):
            heads = (2 * pair, 2 * pair + 1)
            at = slice(pair * 128, pair * 128 + 128)
            spread = [jnp.broadcast_to(cumulative[:, h : h + 1], (ROWS, 128)) for h in heads]
            sizes = [jnp.broadcast_to(step_size[:, h : h + 1], (ROWS, 128)) for h in heads]
            each = jnp.where(first_half, spread[0], spread[1])
            values = inner_conv[micro, :, at].astype(F32)
            weighting = jnp.exp(each[ROWS - 1 :, :] - each) * jnp.where(first_half, sizes[0], sizes[1])
            state = dot(turned, (values * weighting).astype(BF16))
            sent[micro, :, :, at] = state.reshape(SEQ, OWNED, 128).astype(BF16)
            growth[micro, :, at] = jnp.exp(each)

    distances = (4, 3, 5, 2, 6, 1, 7, 0)
    others = [
        lax.rem(place // 2 + step, SEQ // 2) * 2 + side
        for step in distances
        for side in range(2)
    ]

    def decay_to(micro, owner):
        index = micro * SEQ
        return remote(
            decay.at[micro], decays.at[micro, place], decay_s.at[index + owner], decay_r.at[index + place],
            {"seq": owner},
        )

    def state_to(micro, owner):
        index = micro * SEQ
        return remote(
            sent.at[micro, owner], arrived.at[micro, place], state_s.at[index + owner], state_r.at[index + place],
            {"seq": owner},
        )

    def enter_to(micro, target):
        index = micro * SEQ
        return remote(
            back.at[micro, target], entering.at[micro, place], enter_s.at[index + target], enter_r.at[index + place],
            {"seq": target},
        )

    def incoming(micro, source):
        index = micro * SEQ + source
        to = {"seq": source}
        return (
            remote(decay.at[micro], decays.at[micro, source], decay_s.at[index], decay_r.at[index], to),
            remote(sent.at[micro, source], arrived.at[micro, source], state_s.at[index], state_r.at[index], to),
        )

    def send_states(micro):
        for owner in others:

            @pl.when(jnp.logical_and(place != owner, place < SEQ - 1))
            def _():
                decay_to(micro, owner).start()
                state_to(micro, owner).start()

    def gate(micro):
        raw = (dot(xg[micro], wg[...]) * scales[micro]).astype(BF16).astype(F32)
        gate_act[micro] = silu(raw)

    def inside(micro):
        cumulative, step_size = sums[micro], steps[micro]
        across_step, across_sum = step_size.T, cumulative.T
        scores = dot_turned(state_conv[micro, :, STATE:], state_conv[micro, :, 0:STATE])
        for pair in range(HEADS // 2):
            at = slice(pair * 128, pair * 128 + 128)
            values = inner_conv[micro, :, at]
            parts = []
            for h in (2 * pair, 2 * pair + 1):
                column = jnp.broadcast_to(cumulative[:, h : h + 1], (ROWS, 128))
                fade = jnp.exp(jnp.where(later, column - across_sum[h : h + 1, :], -jnp.inf))
                mixing = (scores * fade * across_step[h : h + 1, :]).astype(BF16)
                parts.append(dot(mixing, values))
            skips = [jnp.broadcast_to(skip_scale[:, h : h + 1], (1, 128)) for h in (2 * pair, 2 * pair + 1)]
            skip = jnp.where(first_half[0:1], skips[0], skips[1])
            mixed[micro, :, at] = jnp.where(first_half, parts[0], parts[1]) + skip * values.astype(F32)

    head_of = lax.broadcasted_iota(jnp.int32, (128, LOCAL), 1) // 64
    expand = (head_of == lax.broadcasted_iota(jnp.int32, (128, LOCAL), 0)).astype(F32)

    def scan(micro):
        arrived[micro, place] = sent[micro, place]
        decays[micro, place] = decay[micro]
        for source in range(SEQ - 1):

            @pl.when(place != source)
            def _():
                for copy in incoming(micro, source):
                    copy.wait_recv()

        rows = jnp.concatenate([decays[micro, source] for source in range(SEQ)], axis=0)
        factors = dot(rows, expand, precision=HIGHEST)
        carried = jnp.zeros((OWNED, LOCAL), F32)
        for source in range(SEQ - 1):
            carried = factors[source : source + 1, :] * carried + arrived[micro, source].astype(F32)
            back[micro, source + 1] = carried.astype(BF16)

        for target in others:

            @pl.when(jnp.logical_and(place != target, target > 0))
            def _():
                enter_to(micro, target).start()

        @pl.when(place > 0)
        def _():
            entering[micro, place] = back[micro, place]

    def across(micro):
        for owner in range(SEQ):

            @pl.when(jnp.logical_and(place != owner, place > 0))
            def _():
                index = micro * SEQ + owner
                remote(
                    back.at[micro, owner], entering.at[micro, owner], enter_s.at[index], enter_r.at[index],
                    {"seq": owner},
                ).wait_recv()

        from_state = state_conv[micro, :, STATE:]
        square = jnp.zeros((ROWS, 128), F32)
        for column in range(0, LOCAL, 128):
            at = slice(column, column + 128)
            entry = entering[micro, :, :, at].astype(F32).reshape(STATE, 128).astype(BF16)
            value = mixed[micro, :, at] + growth[micro, :, at] * dot(from_state, entry)
            gated = value * gate_act[micro, :, at]
            square = square + gated * gated
            normed[micro, :, at] = (gated * inner_gain[:, at]).astype(BF16)
        return jnp.sum(square.T, axis=0, keepdims=True)

    spare_row = lax.broadcasted_iota(jnp.int32, (16, ROWS), 0)

    def split(total):
        high = total.astype(BF16).astype(F32)
        return jnp.where(spare_row < 8, high, total - high).astype(BF16)

    def half(micro, which):
        index = micro * CHIPS + which
        return remote(
            halves.at[micro, which, 1 - core], partner_half.at[micro, which], half_s.at[index], half_r.at[index],
            to_partner,
        )

    def spread(micro, total, which):
        at = pl.ds(pl.multiple_of(which * PAIR, 128), PAIR)
        product = dot(normed[micro], wo[:, at]).T
        spare = split(total)
        for side in range(2):
            halves[micro, which, side, 0:NARROW, :] = product[side * NARROW : (side + 1) * NARROW, :].astype(BF16)
            halves[micro, which, side, NARROW:SLAB, :] = spare
        half(micro, which).start()

    def unpacked(block, part):
        wide = block.astype(F32)
        if part == 0:
            return (wide,)
        rest = NARROW - HALF
        return wide[0:rest], wide[rest : rest + 1] + wide[rest + 8 : rest + 9]

    def added(*terms):
        return tuple(sum(values[1:], values[0]) for values in zip(*terms))

    def join(micro, which, part):
        rows = PARTS[part]
        return added(
            unpacked(halves[micro, which, core, rows], part), unpacked(partner_half[micro, which, rows], part)
        )

    def pack(micro, which, part, value):
        if part == 0:
            joined[micro, which, EARLY, :] = value[0].astype(BF16)
        else:
            joined[micro, which, LATE, :] = value[0].astype(BF16)
            joined[micro, which, NARROW:SLAB, :] = split(value[1])

    ways = (after, behind)

    def send_before(micro, part):
        rows, index = PARTS[part], micro * 2 + part
        return remote(
            joined.at[micro, across_ring, rows], before.at[micro, rows], before_s.at[index], before_r.at[index],
            device(ways[part]),
        )

    def send_total(micro, way, part):
        rows, index = PARTS[part], (micro * 2 + way) * 2 + part
        return remote(
            joined.at[micro, ways[way], rows], totals.at[micro, way, rows], total_s.at[index], total_r.at[index],
            device(ways[way]),
        )

    def join_before(micro):
        half(micro, across_ring).wait_recv()
        for part in range(2):
            pack(micro, across_ring, part, join(micro, across_ring, part))
            send_before(micro, part).start()

    def join_direct(micro, way):
        which, part = ways[way], 1 - way
        half(micro, which).wait_recv()
        pack(micro, which, part, join(micro, which, part))
        send_total(micro, way, part).start()

    def join_second(micro):
        for part in range(2):
            which = ways[part]
            value = join(micro, which, part)
            send_before(micro, part).wait_recv()
            pack(micro, which, part, added(value, unpacked(before[micro, PARTS[part]], part)))
            send_total(micro, part, part).start()

    def finish(micro):
        half(micro, chip).wait_recv()
        values = [join(micro, chip, part) for part in range(2)]
        for way, part in ((0, 1), (1, 0), (0, 0), (1, 1)):
            send_total(micro, way, part).wait_recv()
            values[part] = added(values[part], unpacked(totals[micro, way, PARTS[part]], part))
        scale = lax.rsqrt(values[1][1] / INNER + EPS)
        for part, rows in enumerate((EARLY, LATE)):
            result = (x[chip, micro, core, rows].astype(F32) + values[part][0] * scale).astype(BF16)
            own[micro, rows] = result
            out[0, micro, rows] = result

            @pl.when(section == 0)
            def _():
                handover(micro, part).start()

    scope = jax.named_scope
    with scope("own"):
        send_loaded(0)
        send_loaded(1)
        send_passed(0)
    for load in loads[MICRO:12]:
        load.wait()
    with scope("near0"):
        forward_near(0)
    with scope("p0"):
        project(0, chip, True)
        project(0, behind, False)
        project(0, after, False)
    with scope("far0"):
        forward_far(0)
        project(0, across_ring, False)
        project_end(0)
    with scope("own1"):
        send_passed(1)
    with scope("near1"):
        forward_near(1)
    with scope("p1"):
        project(1, chip, True)
        project(1, behind, False)
        project(1, after, False)
    with scope("states0"):
        states(0)
        send_states(0)
    with scope("far1"):
        forward_far(1)
        project(1, across_ring, False)
        project_end(1)
    for load in loads[12:]:
        load.wait()
    with scope("fill0"):
        gate(0)
        inside(0)
    with scope("states1"):
        states(1)
        send_states(1)
    with scope("fill1"):
        gate(1)
        inside(1)
    with scope("scan0"):
        scan(0)
    with scope("scan1"):
        scan(1)
    with scope("across0"):
        total = across(0)
    with scope("spread0"):
        spread(0, total, across_ring)
        spread(0, total, after)
        spread(0, total, behind)
        join_before(0)
    with scope("across1"):
        total1 = across(1)
    with scope("spread1"):
        spread(1, total1, across_ring)
        join_direct(0, 0)
        spread(1, total1, after)
        join_direct(0, 1)
        join_before(1)
        spread(0, total, chip)
    with scope("second0"):
        join_second(0)
        spread(1, total1, behind)
        join_direct(1, 0)
        spread(1, total1, chip)
        join_direct(1, 1)
    with scope("finish0"):
        finish(0)
    with scope("sent"):
        for micro in range(MICRO):
            for send in range(SENDS):
                gather(micro, send).wait_send()

            @pl.when(place < SEQ - 1)
            def _():
                rim(micro).wait_send()

            for owner in range(SEQ):

                @pl.when(jnp.logical_and(place != owner, place < SEQ - 1))
                def _():
                    decay_to(micro, owner).wait_send()
                    state_to(micro, owner).wait_send()

                if owner > 0:

                    @pl.when(place != owner)
                    def _():
                        enter_to(micro, owner).wait_send()

    with scope("second1"):
        join_second(1)
    with scope("finish1"):
        finish(1)

    for micro in range(MICRO):
        for which in (across_ring, after, behind, chip):
            half(micro, which).wait_send()
        for part in range(2):
            send_before(micro, part).wait_send()
            for way in range(2):
                send_total(micro, way, part).wait_send()

        @pl.when(section == 0)
        def _():
            for part in range(2):
                handover(micro, part).wait_send()


def shards(
    tokens, pre_gain, gate_w, inner_w, state_w, step_w, inner_taps, state_taps, step_bias, decay_rate, skip_scale,
    inner_gain, out_w,
):
    hbm = pl.BlockSpec(memory_space=pltpu.HBM)
    dma = lambda count: pltpu.SemaphoreType.DMA((count,))
    result = pl.pallas_call(
        kernel,
        out_shape=pltpu.VMEM((1, MICRO, NARROW, ROWS), BF16),
        in_specs=[hbm] * 13,
        out_specs=pl.BlockSpec(memory_space=pltpu.VMEM),
        scratch_shapes=[
            pltpu.VMEM((CHIPS, MICRO, 2, NARROW, ROWS), BF16),
            pltpu.VMEM((MICRO, ROWS, WIDTH), BF16),
            pltpu.VMEM((WIDTH, BOTH), BF16),
            pltpu.VMEM((HEADS, WIDTH), BF16),
            pltpu.VMEM((WIDTH, LOCAL), BF16),
            pltpu.VMEM((LOCAL, WIDTH), BF16),
            pltpu.VMEM((1, WIDTH), F32),
            pltpu.VMEM((TAPS + 1, 1, LOCAL), F32),
            pltpu.VMEM((TAPS + 1, 1, 2 * STATE), F32),
            pltpu.VMEM((1, HEADS), F32),
            pltpu.VMEM((1, HEADS), F32),
            pltpu.VMEM((1, HEADS), F32),
            pltpu.VMEM((1, LOCAL), F32),
            pltpu.VMEM((MICRO, ROWS, BOTH), F32),
            pltpu.VMEM((MICRO, ROWS, HEADS), F32),
            pltpu.VMEM((MICRO, ROWS, LOCAL), F32),
            pltpu.VMEM((MICRO, ROWS, 128), F32),
            pltpu.VMEM((MICRO, ROWS, 1), F32),
            pltpu.VMEM((MICRO, EDGE + ROWS, BOTH), F32),
            pltpu.VMEM((MICRO, ROWS, LOCAL), BF16),
            pltpu.VMEM((MICRO, ROWS, 2 * STATE), BF16),
            pltpu.VMEM((MICRO, ROWS, 128), F32),
            pltpu.VMEM((MICRO, ROWS, 128), F32),
            pltpu.VMEM((MICRO, ROWS, LOCAL), F32),
            pltpu.VMEM((MICRO, ROWS, LOCAL), F32),
            pltpu.VMEM((MICRO, 1, 128), F32),
            pltpu.VMEM((MICRO, SEQ, 1, 128), F32),
            pltpu.VMEM((MICRO, SEQ, OWNED, LOCAL), BF16),
            pltpu.VMEM((MICRO, SEQ, OWNED, LOCAL), BF16),
            pltpu.VMEM((MICRO, SEQ, OWNED, LOCAL), BF16),
            pltpu.VMEM((MICRO, SEQ, OWNED, LOCAL), BF16),
            pltpu.VMEM((MICRO, ROWS, LOCAL), BF16),
            pltpu.VMEM((MICRO, CHIPS, 2, SLAB, ROWS), BF16),
            pltpu.VMEM((MICRO, CHIPS, SLAB, ROWS), BF16),
            pltpu.VMEM((MICRO, CHIPS, SLAB, ROWS), BF16),
            pltpu.VMEM((MICRO, SLAB, ROWS), BF16),
            pltpu.VMEM((MICRO, 2, SLAB, ROWS), BF16),
            pltpu.VMEM((MICRO, NARROW, ROWS), BF16),
            dma(14), dma(MICRO * SENDS), dma(CHIPS * MICRO * 2), dma(CHIPS * MICRO), dma(MICRO), dma(MICRO),
            dma(MICRO * SEQ), dma(MICRO * SEQ), dma(MICRO * SEQ), dma(MICRO * SEQ), dma(MICRO * SEQ), dma(MICRO * SEQ),
            dma(MICRO * CHIPS), dma(MICRO * CHIPS), dma(MICRO * 2), dma(MICRO * 2), dma(MICRO * 4), dma(MICRO * 4),
            dma(MICRO * 2), dma(MICRO * 2),
        ],
        compiler_params=pltpu.CompilerParams(
            collective_id=0, has_side_effects=True, vmem_limit_bytes=56 * 1024 * 1024
        ),
    )(
        jnp.swapaxes(tokens, 1, 2), pre_gain, gate_w, inner_w, state_w, jnp.swapaxes(step_w, 1, 2),
        jnp.swapaxes(inner_taps, 0, 1), jnp.swapaxes(state_taps, 0, 1), step_bias, decay_rate, skip_scale, inner_gain,
        out_w,
    )
    return jnp.swapaxes(result, 2, 3)


def solution(mesh):
    return jax.shard_map(
        shards,
        mesh=mesh,
        in_specs=(
            P(None, "seq", "tensor"),
            P("pipe", None),
            P("pipe", None, "tensor"),
            P("pipe", None, "tensor"),
            P("pipe", None, None),
            P("pipe", None, "tensor"),
            P("pipe", None, "tensor"),
            P("pipe", None, None),
            P("pipe", "tensor"),
            P("pipe", "tensor"),
            P("pipe", "tensor"),
            P("pipe", "tensor"),
            P("pipe", "tensor", None),
        ),
        out_specs=P("pipe", None, "seq", "tensor"),
        check_vma=False,
    )
```

```python
import jax
import jax.numpy as jnp
from jax import lax
from jax.experimental import pallas as pl
from jax.experimental.pallas import tpu as pltpu
from jax.sharding import PartitionSpec as P

MESH = pl.DeviceIdType.MESH
F32, BF16 = jnp.float32, jnp.bfloat16
HIGHEST = lax.Precision.HIGHEST
EPS = 1e-05
SHARE, SEQ = 8, 16
CHIPS = SHARE // 2
MICRO, ROWS, WIDTH, INNER = 2, 128, 2560, 5120
NARROW = WIDTH // SHARE
PAIR = 2 * NARROW
LOCAL = INNER // SHARE
STATE = 128
BOTH = LOCAL + 2 * STATE
HEADS = 10
TAPS = 4
SLAB = NARROW + 16
OWNED = STATE // SEQ
EDGE = 8
HALF = NARROW // 2
SENDS = 10
NEAR = 4
EARLY, LATE = slice(0, HALF), slice(HALF, NARROW)
PARTS = (slice(0, HALF), slice(HALF, SLAB))


def silu(value):
    return value / (1.0 + jnp.exp(-value))


def dot(a, b, **options):
    return jnp.dot(a, b, preferred_element_type=F32, **options)


def dot_turned(a, b):
    return lax.dot_general(a, b, (((1,), (1,)), ((), ())), preferred_element_type=F32)


def remote(src, dst, send, recv, device):
    return pltpu.make_async_remote_copy(
        src_ref=src, dst_ref=dst, send_sem=send, recv_sem=recv, device_id=device, device_id_type=MESH
    )


def kernel(
    tokens, pre_gain_h, gate_h, inner_h, state_h, step_h, inner_taps_h, state_taps_h, bias_h, rate_h, skip_h, gain_h,
    out_h, out,
    x, xg, w1, wd, wg, wo, pre_gain, inner_taps, state_taps, bias, rate, skip_scale, inner_gain,
    acc, acc_d, gate_act, squares, scales, padded, inner_conv, state_conv, steps, sums, growth, mixed, decay, decays, sent,
    arrived, back, entering, normed, halves, partner_half, joined, before, totals, own,
    local_s, gather_s, gather_r, share_r, rim_s, rim_r, decay_s, decay_r, state_s, state_r, enter_s, enter_r, half_s, half_r,
    before_s, before_r, total_s, total_r, pipe_s, pipe_r,
):
    section, member, place = (lax.axis_index(name) for name in ("pipe", "tensor", "seq"))
    chip, core = member // 2, member % 2
    partner = member + 1 - 2 * core
    after, behind, across_ring = (lax.rem(chip + step, CHIPS) for step in (1, CHIPS - 1, 2))

    def device(which):
        return {"tensor": which * 2 + core}

    loads = [
        pltpu.make_async_copy(source, target, local_s.at[index])
        for index, (source, target) in enumerate(
            (
                (tokens.at[0], x.at[chip, 0, core]),
                (tokens.at[1], x.at[chip, 1, core]),
                (inner_h.at[0], w1.at[:, 0:LOCAL]),
                (state_h.at[0], w1.at[:, LOCAL:BOTH]),
                (step_h.at[0], wd),
                (pre_gain_h, pre_gain),
                (inner_taps_h, inner_taps),
                (state_taps_h, state_taps),
                (bias_h, bias),
                (rate_h, rate),
                (skip_h, skip_scale),
                (gain_h, inner_gain),
                (gate_h.at[0], wg),
                (out_h.at[0], wo),
            )
        )
    ]

    @pl.when(section == 0)
    def _():
        for load in loads[:MICRO]:
            load.start()

    for load in loads[MICRO:]:
        load.start()

    barrier = pltpu.get_barrier_semaphore()

    def greet(peer):
        pl.semaphore_signal(barrier, inc=1, device_id=peer, device_id_type=MESH)

    for step in range(1, SEQ):
        greet({"seq": lax.rem(place + step, SEQ)})
    greet({"pipe": 1 - section})
    greet(device(after))
    greet(device(behind))
    greet({"tensor": partner})

    steps[...] = jnp.zeros_like(steps)

    @pl.when(place == 0)
    def _():
        padded[:, 0:EDGE, :] = jnp.zeros((MICRO, EDGE, BOTH), F32)
        entering[...] = jnp.zeros_like(entering)

    pl.semaphore_wait(barrier, SEQ - 1 + 4)

    def handover(micro, part):
        rows = (EARLY, LATE)[part]
        return remote(
            own.at[micro, rows], x.at[chip, micro, core, rows], pipe_s.at[0], pipe_r.at[micro], {"pipe": 1}
        )

    def handed_over(micro):
        return remote(own.at[micro], x.at[chip, micro, core], pipe_s.at[0], pipe_r.at[micro], {"pipe": 1})

    to_partner = {"tensor": partner}

    def gather(micro, send):
        which, part, target = (
            (chip, 0, after),
            (chip, 1, behind),
            (chip, 1, after),
            (chip, 0, behind),
            (behind, 0, after),
            (after, 1, behind),
            (chip, 2, None),
            (behind, 2, None),
            (after, 2, None),
            (across_ring, 2, None),
        )[send]
        if part == 2:
            block = x.at[which, micro, core]
            return remote(block, block, gather_s.at[1], share_r.at[which * MICRO + micro], to_partner)
        block = x.at[which, micro, core, (EARLY, LATE)[part]]
        slot = NEAR * MICRO + micro if send in (4, 5) else micro * NEAR + (0, 3, 1, 2)[send]
        return remote(block, block, gather_s.at[0], gather_r.at[slot], device(target))

    def near(micro, which, part, slot):
        block = x.at[which, micro, core, (EARLY, LATE)[part]]
        return remote(block, block, gather_s.at[0], gather_r.at[micro * NEAR + slot], to_partner)

    def far(micro):
        block = x.at[across_ring, micro, core]
        return remote(block, block, gather_s.at[0], gather_r.at[NEAR * MICRO + micro], to_partner)

    def shared(micro, which):
        block = x.at[which, micro, 1 - core]
        return remote(block, block, gather_s.at[1], share_r.at[which * MICRO + micro], to_partner)

    def start_own(micro):
        for send in (0, 1, 2, 3, 6):
            gather(micro, send).start()

    def send_loaded(micro):
        @pl.when(section == 0)
        def _():
            loads[micro].wait()
            start_own(micro)

    def send_passed(micro):
        @pl.when(section == 1)
        def _():
            handed_over(micro).wait_recv()
            start_own(micro)

    def forward_near(micro):
        near(micro, behind, 0, 0).wait_recv()
        gather(micro, 4).start()
        near(micro, after, 1, 3).wait_recv()
        gather(micro, 5).start()
        near(micro, behind, 1, 1).wait_recv()
        gather(micro, 7).start()
        near(micro, after, 0, 2).wait_recv()
        gather(micro, 8).start()

    def forward_far(micro):
        far(micro).wait_recv()
        gather(micro, 9).start()

    def project(micro, which, first):
        shared(micro, which).wait_recv()
        wide = x[which, micro].reshape(PAIR, ROWS).astype(F32).T
        at = pl.ds(pl.multiple_of(which * PAIR, 128), PAIR)
        scaled = (wide * pre_gain[:, at]).astype(BF16)
        xg[micro, :, at] = scaled
        square = wide * wide
        square = sum(square[:, column : column + 128] for column in range(0, PAIR, 128))
        term = dot(scaled, w1[at, :])
        term_d = dot_turned(scaled, wd[:, at])
        if first:
            acc[micro], acc_d[micro], squares[micro] = term, term_d, square
        else:
            acc[micro] += term
            acc_d[micro] += term_d
            squares[micro] += square

    def rim(micro):
        return remote(
            padded.at[micro, ROWS : ROWS + EDGE, :], padded.at[micro, 0:EDGE, :], rim_s.at[micro], rim_r.at[micro],
            {"seq": lax.rem(place + 1, SEQ)},
        )

    def project_end(micro):
        scale = lax.rsqrt(jnp.sum(squares[micro], axis=1, keepdims=True) / WIDTH + EPS)
        scales[micro] = scale
        padded[micro, EDGE : EDGE + ROWS, :] = (acc[micro] * scale).astype(BF16).astype(F32)

        @pl.when(place < SEQ - 1)
        def _():
            rim(micro).start()

        shifted = acc_d[micro] * scale + bias[...]
        steps[micro, :, 0:HEADS] = jnp.maximum(shifted, 0.0) + jnp.log1p(jnp.exp(-jnp.abs(shifted)))

    row = lax.broadcasted_iota(jnp.int32, (ROWS, ROWS), 0)
    lane = lax.broadcasted_iota(jnp.int32, (ROWS, ROWS), 1)
    first_half = lane < 64
    later = row >= lane

    def states(micro):
        rates = jnp.concatenate([rate[...], jnp.zeros((1, 128 - HEADS), F32)], axis=1)
        step_size = steps[micro]
        cumulative = dot(later.astype(F32), -step_size * rates, precision=HIGHEST)
        sums[micro] = cumulative
        decay[micro] = jnp.exp(cumulative[ROWS - 1 :, :])

        @pl.when(place > 0)
        def _():
            rim(micro).wait_recv()

        for column in range(0, BOTH, 128):
            taps, at = (inner_taps, column) if column < LOCAL else (state_taps, column - LOCAL)
            total = jnp.broadcast_to(taps[TAPS, :, at : at + 128], (ROWS, 128))
            for index in range(TAPS):
                begin = EDGE - TAPS + 1 + index
                total = total + taps[index, :, at : at + 128] * (
                    padded[micro, begin : begin + ROWS, column : column + 128]
                )
            result = silu(total).astype(BF16)
            if column < LOCAL:
                inner_conv[micro, :, at : at + 128] = result
            else:
                state_conv[micro, :, at : at + 128] = result

        turned = state_conv[micro, :, 0:STATE].astype(F32).T.astype(BF16)
        for pair in range(HEADS // 2):
            heads = (2 * pair, 2 * pair + 1)
            at = slice(pair * 128, pair * 128 + 128)
            spread = [jnp.broadcast_to(cumulative[:, h : h + 1], (ROWS, 128)) for h in heads]
            sizes = [jnp.broadcast_to(step_size[:, h : h + 1], (ROWS, 128)) for h in heads]
            each = jnp.where(first_half, spread[0], spread[1])
            values = inner_conv[micro, :, at].astype(F32)
            weighting = jnp.exp(each[ROWS - 1 :, :] - each) * jnp.where(first_half, sizes[0], sizes[1])
            state = dot(turned, (values * weighting).astype(BF16))
            sent[micro, :, :, at] = state.reshape(SEQ, OWNED, 128).astype(BF16)
            growth[micro, :, at] = jnp.exp(each)

    distances = (4, 3, 5, 2, 6, 1, 7, 0)
    others = [
        lax.rem(place // 2 + step, SEQ // 2) * 2 + side
        for step in distances
        for side in range(2)
    ]

    def decay_to(micro, owner):
        return remote(
            decay.at[micro], decays.at[micro, place], decay_s.at[micro], decay_r.at[micro], {"seq": owner}
        )

    def state_to(micro, owner):
        return remote(
            sent.at[micro, owner], arrived.at[micro, place], state_s.at[micro], state_r.at[micro], {"seq": owner}
        )

    def enter_to(micro, target):
        return remote(
            back.at[micro, target], entering.at[micro, place], enter_s.at[micro], enter_r.at[micro], {"seq": target}
        )

    def all_decays(micro, count):
        block = decays.at[micro, 0:count]
        return remote(block, block, decay_s.at[micro], decay_r.at[micro], to_partner)

    def all_states(micro, count):
        block = arrived.at[micro, 0:count]
        return remote(block, block, state_s.at[micro], state_r.at[micro], to_partner)

    def all_entering(micro, count):
        block = entering.at[micro, 0:count]
        return remote(block, block, enter_s.at[micro], enter_r.at[micro], to_partner)

    def send_states(micro):
        for owner in others:

            @pl.when(jnp.logical_and(place != owner, place < SEQ - 1))
            def _():
                decay_to(micro, owner).start()
                state_to(micro, owner).start()

    def gate(micro):
        raw = (dot(xg[micro], wg[...]) * scales[micro]).astype(BF16).astype(F32)
        gate_act[micro] = silu(raw)

    def inside(micro):
        cumulative, step_size = sums[micro], steps[micro]
        across_step, across_sum = step_size.T, cumulative.T
        scores = dot_turned(state_conv[micro, :, STATE:], state_conv[micro, :, 0:STATE])
        for pair in range(HEADS // 2):
            at = slice(pair * 128, pair * 128 + 128)
            values = inner_conv[micro, :, at]
            parts = []
            for h in (2 * pair, 2 * pair + 1):
                column = jnp.broadcast_to(cumulative[:, h : h + 1], (ROWS, 128))
                fade = jnp.exp(jnp.where(later, column - across_sum[h : h + 1, :], -jnp.inf))
                mixing = (scores * fade * across_step[h : h + 1, :]).astype(BF16)
                parts.append(dot(mixing, values))
            skips = [jnp.broadcast_to(skip_scale[:, h : h + 1], (1, 128)) for h in (2 * pair, 2 * pair + 1)]
            skip = jnp.where(first_half[0:1], skips[0], skips[1])
            mixed[micro, :, at] = jnp.where(first_half, parts[0], parts[1]) + skip * values.astype(F32)

    head_of = lax.broadcasted_iota(jnp.int32, (128, LOCAL), 1) // 64
    expand = (head_of == lax.broadcasted_iota(jnp.int32, (128, LOCAL), 0)).astype(F32)

    def scan(micro):
        arrived[micro, place] = sent[micro, place]
        decays[micro, place] = decay[micro]
        @pl.when(place < SEQ - 1)
        def _():
            all_decays(micro, SEQ - 2).wait_recv()
            all_states(micro, SEQ - 2).wait_recv()

        @pl.when(place == SEQ - 1)
        def _():
            all_decays(micro, SEQ - 1).wait_recv()
            all_states(micro, SEQ - 1).wait_recv()

        rows = jnp.concatenate([decays[micro, source] for source in range(SEQ)], axis=0)
        factors = dot(rows, expand, precision=HIGHEST)
        carried = jnp.zeros((OWNED, LOCAL), F32)
        for source in range(SEQ - 1):
            carried = factors[source : source + 1, :] * carried + arrived[micro, source].astype(F32)
            back[micro, source + 1] = carried.astype(BF16)

        for target in others:

            @pl.when(jnp.logical_and(place != target, target > 0))
            def _():
                enter_to(micro, target).start()

        @pl.when(place > 0)
        def _():
            entering[micro, place] = back[micro, place]

    def across(micro):
        @pl.when(place > 0)
        def _():
            all_entering(micro, SEQ - 1).wait_recv()

        from_state = state_conv[micro, :, STATE:]
        square = jnp.zeros((ROWS, 128), F32)
        for column in range(0, LOCAL, 128):
            at = slice(column, column + 128)
            entry = entering[micro, :, :, at].astype(F32).reshape(STATE, 128).astype(BF16)
            value = mixed[micro, :, at] + growth[micro, :, at] * dot(from_state, entry)
            gated = value * gate_act[micro, :, at]
            square = square + gated * gated
            normed[micro, :, at] = (gated * inner_gain[:, at]).astype(BF16)
        return jnp.sum(square.T, axis=0, keepdims=True)

    spare_row = lax.broadcasted_iota(jnp.int32, (16, ROWS), 0)

    def split(total):
        high = total.astype(BF16).astype(F32)
        return jnp.where(spare_row < 8, high, total - high).astype(BF16)

    def half(micro, which):
        index = micro * CHIPS + which
        return remote(
            halves.at[micro, which, 1 - core], partner_half.at[micro, which], half_s.at[0], half_r.at[index],
            to_partner,
        )

    def spread(micro, total, which):
        at = pl.ds(pl.multiple_of(which * PAIR, 128), PAIR)
        product = dot(normed[micro], wo[:, at]).T
        spare = split(total)
        for side in range(2):
            halves[micro, which, side, 0:NARROW, :] = product[side * NARROW : (side + 1) * NARROW, :].astype(BF16)
            halves[micro, which, side, NARROW:SLAB, :] = spare
        half(micro, which).start()

    def unpacked(block, part):
        wide = block.astype(F32)
        if part == 0:
            return (wide,)
        rest = NARROW - HALF
        return wide[0:rest], wide[rest : rest + 1] + wide[rest + 8 : rest + 9]

    def added(*terms):
        return tuple(sum(values[1:], values[0]) for values in zip(*terms))

    def join(micro, which, part):
        rows = PARTS[part]
        return added(
            unpacked(halves[micro, which, core, rows], part), unpacked(partner_half[micro, which, rows], part)
        )

    def pack(micro, which, part, value):
        if part == 0:
            joined[micro, which, EARLY, :] = value[0].astype(BF16)
        else:
            joined[micro, which, LATE, :] = value[0].astype(BF16)
            joined[micro, which, NARROW:SLAB, :] = split(value[1])

    ways = (after, behind)

    def send_before(micro, part):
        rows, index = PARTS[part], micro * 2 + part
        return remote(
            joined.at[micro, across_ring, rows], before.at[micro, rows], before_s.at[0], before_r.at[index],
            device(ways[part]),
        )

    def send_total(micro, way, part):
        rows = PARTS[part]
        return remote(
            joined.at[micro, ways[way], rows], totals.at[micro, way, rows], total_s.at[0], total_r.at[micro],
            device(ways[way]),
        )

    def every(block, send, recv):
        return remote(block, block, send, recv, to_partner)

    def join_before(micro):
        half(micro, across_ring).wait_recv()
        for part in range(2):
            pack(micro, across_ring, part, join(micro, across_ring, part))
            send_before(micro, part).start()

    def join_direct(micro, way):
        which, part = ways[way], 1 - way
        half(micro, which).wait_recv()
        pack(micro, which, part, join(micro, which, part))
        send_total(micro, way, part).start()

    def join_second(micro):
        for part in range(2):
            which = ways[part]
            value = join(micro, which, part)
            send_before(micro, part).wait_recv()
            pack(micro, which, part, added(value, unpacked(before[micro, PARTS[part]], part)))
            send_total(micro, part, part).start()

    def finish(micro):
        half(micro, chip).wait_recv()
        values = [join(micro, chip, part) for part in range(2)]
        every(totals.at[micro], total_s.at[0], total_r.at[micro]).wait_recv()
        for way, part in ((0, 1), (1, 0), (0, 0), (1, 1)):
            values[part] = added(values[part], unpacked(totals[micro, way, PARTS[part]], part))
        scale = lax.rsqrt(values[1][1] / INNER + EPS)
        for part, rows in enumerate((EARLY, LATE)):
            result = (x[chip, micro, core, rows].astype(F32) + values[part][0] * scale).astype(BF16)
            own[micro, rows] = result
            out[0, micro, rows] = result

            @pl.when(section == 0)
            def _():
                handover(micro, part).start()

    scope = jax.named_scope
    with scope("own"):
        send_loaded(0)
        send_loaded(1)
        send_passed(0)
    for load in loads[MICRO:12]:
        load.wait()
    with scope("near0"):
        forward_near(0)
    with scope("p0"):
        project(0, chip, True)
        project(0, behind, False)
    with scope("own1"):
        send_passed(1)
        project(0, after, False)

    @pl.when(section == 0)
    def _():
        forward_near(1)

    with scope("far0"):
        forward_far(0)
        project(0, across_ring, False)
        project_end(0)

    @pl.when(section == 1)
    def _():
        forward_near(1)

    with scope("p1"):
        project(1, chip, True)
        project(1, behind, False)
        project(1, after, False)
    with scope("states0"):
        states(0)
        send_states(0)
    with scope("far1"):
        forward_far(1)
        project(1, across_ring, False)
        project_end(1)
    for load in loads[12:]:
        load.wait()
    with scope("fill0"):
        gate(0)
        inside(0)
    with scope("states1"):
        states(1)
        send_states(1)
    with scope("fill1"):
        gate(1)
        inside(1)
    with scope("scan0"):
        scan(0)
    with scope("scan1"):
        scan(1)
    with scope("across0"):
        total = across(0)
    with scope("spread0"):
        spread(0, total, across_ring)
        spread(0, total, after)
        spread(0, total, behind)
        join_before(0)
    with scope("across1"):
        total1 = across(1)
    with scope("spread1"):
        spread(1, total1, across_ring)
        join_direct(0, 0)
        spread(1, total1, after)
        join_direct(0, 1)
        join_before(1)
        spread(0, total, chip)
    with scope("second0"):
        join_second(0)
        spread(1, total1, behind)
        join_direct(1, 0)
        spread(1, total1, chip)
        join_direct(1, 1)
    with scope("finish0"):
        finish(0)
    with scope("sent"):
        every(x.at[0:3, 0], gather_s.at[0], share_r.at[0]).wait_send()
        every(x.at[0:2], gather_s.at[1], share_r.at[0]).wait_send()
        for micro in range(MICRO):

            @pl.when(place < SEQ - 1)
            def _():
                rim(micro).wait_send()
                all_decays(micro, SEQ - 1).wait_send()
                all_states(micro, SEQ - 1).wait_send()

            @pl.when(place == 0)
            def _():
                all_entering(micro, SEQ - 1).wait_send()

            @pl.when(place > 0)
            def _():
                all_entering(micro, SEQ - 2).wait_send()

    with scope("second1"):
        join_second(1)
    with scope("finish1"):
        finish(1)

    every(halves.at[0], half_s.at[0], half_r.at[0]).wait_send()
    every(before, before_s.at[0], before_r.at[0]).wait_send()
    every(totals, total_s.at[0], total_r.at[0]).wait_send()

    @pl.when(section == 0)
    def _():
        every(own, pipe_s.at[0], pipe_r.at[0]).wait_send()


def shards(
    tokens, pre_gain, gate_w, inner_w, state_w, step_w, inner_taps, state_taps, step_bias, decay_rate, skip_scale,
    inner_gain, out_w,
):
    hbm = pl.BlockSpec(memory_space=pltpu.HBM)
    dma = lambda count: pltpu.SemaphoreType.DMA((count,))
    result = pl.pallas_call(
        kernel,
        out_shape=pltpu.VMEM((1, MICRO, NARROW, ROWS), BF16),
        in_specs=[hbm] * 13,
        out_specs=pl.BlockSpec(memory_space=pltpu.VMEM),
        scratch_shapes=[
            pltpu.VMEM((CHIPS, MICRO, 2, NARROW, ROWS), BF16),
            pltpu.VMEM((MICRO, ROWS, WIDTH), BF16),
            pltpu.VMEM((WIDTH, BOTH), BF16),
            pltpu.VMEM((HEADS, WIDTH), BF16),
            pltpu.VMEM((WIDTH, LOCAL), BF16),
            pltpu.VMEM((LOCAL, WIDTH), BF16),
            pltpu.VMEM((1, WIDTH), F32),
            pltpu.VMEM((TAPS + 1, 1, LOCAL), F32),
            pltpu.VMEM((TAPS + 1, 1, 2 * STATE), F32),
            pltpu.VMEM((1, HEADS), F32),
            pltpu.VMEM((1, HEADS), F32),
            pltpu.VMEM((1, HEADS), F32),
            pltpu.VMEM((1, LOCAL), F32),
            pltpu.VMEM((MICRO, ROWS, BOTH), F32),
            pltpu.VMEM((MICRO, ROWS, HEADS), F32),
            pltpu.VMEM((MICRO, ROWS, LOCAL), F32),
            pltpu.VMEM((MICRO, ROWS, 128), F32),
            pltpu.VMEM((MICRO, ROWS, 1), F32),
            pltpu.VMEM((MICRO, EDGE + ROWS, BOTH), F32),
            pltpu.VMEM((MICRO, ROWS, LOCAL), BF16),
            pltpu.VMEM((MICRO, ROWS, 2 * STATE), BF16),
            pltpu.VMEM((MICRO, ROWS, 128), F32),
            pltpu.VMEM((MICRO, ROWS, 128), F32),
            pltpu.VMEM((MICRO, ROWS, LOCAL), F32),
            pltpu.VMEM((MICRO, ROWS, LOCAL), F32),
            pltpu.VMEM((MICRO, 1, 128), F32),
            pltpu.VMEM((MICRO, SEQ, 1, 128), F32),
            pltpu.VMEM((MICRO, SEQ, OWNED, LOCAL), BF16),
            pltpu.VMEM((MICRO, SEQ, OWNED, LOCAL), BF16),
            pltpu.VMEM((MICRO, SEQ, OWNED, LOCAL), BF16),
            pltpu.VMEM((MICRO, SEQ, OWNED, LOCAL), BF16),
            pltpu.VMEM((MICRO, ROWS, LOCAL), BF16),
            pltpu.VMEM((MICRO, CHIPS, 2, SLAB, ROWS), BF16),
            pltpu.VMEM((MICRO, CHIPS, SLAB, ROWS), BF16),
            pltpu.VMEM((MICRO, CHIPS, SLAB, ROWS), BF16),
            pltpu.VMEM((MICRO, SLAB, ROWS), BF16),
            pltpu.VMEM((MICRO, 2, SLAB, ROWS), BF16),
            pltpu.VMEM((MICRO, NARROW, ROWS), BF16),
            dma(14), dma(2), dma((NEAR + 1) * MICRO), dma(CHIPS * MICRO), dma(MICRO), dma(MICRO),
            dma(MICRO), dma(MICRO), dma(MICRO), dma(MICRO), dma(MICRO), dma(MICRO),
            dma(1), dma(MICRO * CHIPS), dma(1), dma(MICRO * 2), dma(1), dma(MICRO), dma(1), dma(MICRO),
        ],
        compiler_params=pltpu.CompilerParams(
            collective_id=0, has_side_effects=True, vmem_limit_bytes=56 * 1024 * 1024
        ),
    )(
        jnp.swapaxes(tokens, 1, 2), pre_gain, gate_w, inner_w, state_w, jnp.swapaxes(step_w, 1, 2),
        jnp.swapaxes(inner_taps, 0, 1), jnp.swapaxes(state_taps, 0, 1), step_bias, decay_rate, skip_scale, inner_gain,
        out_w,
    )
    return jnp.swapaxes(result, 2, 3)


def solution(mesh):
    return jax.shard_map(
        shards,
        mesh=mesh,
        in_specs=(
            P(None, "seq", "tensor"),
            P("pipe", None),
            P("pipe", None, "tensor"),
            P("pipe", None, "tensor"),
            P("pipe", None, None),
            P("pipe", None, "tensor"),
            P("pipe", None, "tensor"),
            P("pipe", None, None),
            P("pipe", "tensor"),
            P("pipe", "tensor"),
            P("pipe", "tensor"),
            P("pipe", "tensor"),
            P("pipe", "tensor", None),
        ),
        out_specs=P("pipe", None, "seq", "tensor"),
        check_vma=False,
    )
```

```python
import jax
import jax.numpy as jnp
from jax import lax
from jax.experimental import pallas as pl
from jax.experimental.pallas import tpu as pltpu
from jax.sharding import PartitionSpec as P

MESH = pl.DeviceIdType.MESH
F32, BF16 = jnp.float32, jnp.bfloat16
HIGHEST = lax.Precision.HIGHEST
EPS = 1e-05
SHARE, SEQ = 8, 16
CHIPS = SHARE // 2
MICRO, ROWS, WIDTH, INNER = 2, 128, 2560, 5120
NARROW = WIDTH // SHARE
PAIR = 2 * NARROW
LOCAL = INNER // SHARE
STATE = 128
BOTH = LOCAL + 2 * STATE
WIDE = BOTH + 128
HEADS = 10
TAPS = 4
SLAB = NARROW + 16
OWNED = STATE // SEQ
EDGE = 8
HALF = NARROW // 2
SENDS = 10
NEAR = 4
EARLY, LATE = slice(0, HALF), slice(HALF, NARROW)
PARTS = (slice(0, HALF), slice(HALF, SLAB))


def silu(value):
    return value / (1.0 + jnp.exp(-value))


def dot(a, b, **options):
    return jnp.dot(a, b, preferred_element_type=F32, **options)


def dot_turned(a, b):
    return lax.dot_general(a, b, (((1,), (1,)), ((), ())), preferred_element_type=F32)


def remote(src, dst, send, recv, device):
    return pltpu.make_async_remote_copy(
        src_ref=src, dst_ref=dst, send_sem=send, recv_sem=recv, device_id=device, device_id_type=MESH
    )


def kernel(
    tokens, pre_gain_h, gate_h, inner_h, state_h, step_h, inner_taps_h, state_taps_h, bias_h, rate_h, skip_h, gain_h,
    out_h, out,
    x, xg, w1, wd, wg, wo, pre_gain, inner_taps, state_taps, bias, rate, skip_scale, inner_gain,
    acc, turned_steps, gate_act, squares, scales, padded, inner_conv, state_conv, steps, sums, growth, mixed, decay, decays, sent,
    arrived, back, entering, normed, halves, partner_half, joined, before, totals, own,
    local_s, gather_s, gather_r, share_r, rim_s, rim_r, decay_s, decay_r, state_s, state_r, enter_s, enter_r, half_s, half_r,
    before_s, before_r, total_s, total_r, pipe_s, pipe_r,
):
    section, member, place = (lax.axis_index(name) for name in ("pipe", "tensor", "seq"))
    chip, core = member // 2, member % 2
    partner = member + 1 - 2 * core
    after, behind, across_ring = (lax.rem(chip + step, CHIPS) for step in (1, CHIPS - 1, 2))

    def device(which):
        return {"tensor": which * 2 + core}

    loads = [
        pltpu.make_async_copy(source, target, local_s.at[index])
        for index, (source, target) in enumerate(
            (
                (tokens.at[0], x.at[chip, 0, core]),
                (tokens.at[1], x.at[chip, 1, core]),
                (inner_h.at[0], w1.at[:, 0:LOCAL]),
                (state_h.at[0], w1.at[:, LOCAL:BOTH]),
                (step_h.at[0], wd),
                (pre_gain_h, pre_gain),
                (inner_taps_h, inner_taps),
                (state_taps_h, state_taps),
                (bias_h, bias),
                (rate_h, rate),
                (skip_h, skip_scale),
                (gain_h, inner_gain),
                (gate_h.at[0], wg),
                (out_h.at[0], wo),
            )
        )
    ]

    @pl.when(section == 0)
    def _():
        for load in loads[:MICRO]:
            load.start()

    for load in loads[MICRO:]:
        load.start()

    barrier = pltpu.get_barrier_semaphore()

    def greet(peer):
        pl.semaphore_signal(barrier, inc=1, device_id=peer, device_id_type=MESH)

    for step in range(1, SEQ):
        greet({"seq": lax.rem(place + step, SEQ)})
    greet({"pipe": 1 - section})
    greet(device(after))
    greet(device(behind))
    greet({"tensor": partner})

    steps[...] = jnp.zeros_like(steps)

    @pl.when(place == 0)
    def _():
        padded[:, 0:EDGE, :] = jnp.zeros((MICRO, EDGE, BOTH), F32)
        entering[...] = jnp.zeros_like(entering)

    pl.semaphore_wait(barrier, SEQ - 1 + 4)

    def handover(micro, part):
        rows = (EARLY, LATE)[part]
        return remote(
            own.at[micro, rows], x.at[chip, micro, core, rows], pipe_s.at[0], pipe_r.at[micro], {"pipe": 1}
        )

    def handed_over(micro):
        return remote(own.at[micro], x.at[chip, micro, core], pipe_s.at[0], pipe_r.at[micro], {"pipe": 1})

    to_partner = {"tensor": partner}

    def gather(micro, send):
        which, part, target = (
            (chip, 0, after),
            (chip, 1, behind),
            (chip, 1, after),
            (chip, 0, behind),
            (behind, 0, after),
            (after, 1, behind),
            (chip, 2, None),
            (behind, 2, None),
            (after, 2, None),
            (across_ring, 2, None),
        )[send]
        if part == 2:
            block = x.at[which, micro, core]
            return remote(block, block, gather_s.at[1], share_r.at[which * MICRO + micro], to_partner)
        block = x.at[which, micro, core, (EARLY, LATE)[part]]
        slot = NEAR * MICRO + micro if send in (4, 5) else micro * NEAR + (0, 3, 1, 2)[send]
        return remote(block, block, gather_s.at[0], gather_r.at[slot], device(target))

    def near(micro, which, part, slot):
        block = x.at[which, micro, core, (EARLY, LATE)[part]]
        return remote(block, block, gather_s.at[0], gather_r.at[micro * NEAR + slot], to_partner)

    def far(micro):
        block = x.at[across_ring, micro, core]
        return remote(block, block, gather_s.at[0], gather_r.at[NEAR * MICRO + micro], to_partner)

    def shared(micro, which):
        block = x.at[which, micro, 1 - core]
        return remote(block, block, gather_s.at[1], share_r.at[which * MICRO + micro], to_partner)

    def start_own(micro):
        for send in (0, 1, 2, 3, 6):
            gather(micro, send).start()

    def send_loaded(micro):
        @pl.when(section == 0)
        def _():
            loads[micro].wait()
            start_own(micro)

    def send_passed(micro):
        @pl.when(section == 1)
        def _():
            handed_over(micro).wait_recv()
            start_own(micro)

    def forward_near(micro):
        near(micro, behind, 0, 0).wait_recv()
        gather(micro, 4).start()
        near(micro, after, 1, 3).wait_recv()
        gather(micro, 5).start()
        near(micro, behind, 1, 1).wait_recv()
        gather(micro, 7).start()
        near(micro, after, 0, 2).wait_recv()
        gather(micro, 8).start()

    def forward_far(micro):
        far(micro).wait_recv()
        gather(micro, 9).start()

    def project(micro, which, first):
        shared(micro, which).wait_recv()
        wide = x[which, micro].reshape(PAIR, ROWS).T.astype(F32)
        at = pl.ds(pl.multiple_of(which * PAIR, 128), PAIR)
        scaled = (wide * pre_gain[:, at]).astype(BF16)
        xg[micro, :, at] = scaled
        square = wide * wide
        square = sum(square[:, column : column + 128] for column in range(0, PAIR, 128))
        term = dot(scaled, w1[at, :])
        if first:
            acc[micro], squares[micro] = term, square
        else:
            acc[micro] += term
            squares[micro] += square

    def place_step_weights():
        turned_steps[...] = jnp.zeros_like(turned_steps)
        turned_steps[0:HEADS, :] = wd[...].astype(F32)
        for column in range(0, WIDTH, 128):
            at = slice(column, column + 128)
            w1[at, BOTH : BOTH + 16] = turned_steps[:, at].T.astype(BF16)

    def rim(micro):
        return remote(
            padded.at[micro, ROWS : ROWS + EDGE, :], padded.at[micro, 0:EDGE, :], rim_s.at[micro], rim_r.at[micro],
            {"seq": lax.rem(place + 1, SEQ)},
        )

    def project_end(micro):
        scale = lax.rsqrt(jnp.sum(squares[micro], axis=1, keepdims=True) / WIDTH + EPS)
        scales[micro] = scale
        padded[micro, EDGE : EDGE + ROWS, :] = (acc[micro, :, 0:BOTH] * scale).astype(BF16).astype(F32)

        @pl.when(place < SEQ - 1)
        def _():
            rim(micro).start()

        shifted = acc[micro, :, BOTH : BOTH + HEADS] * scale + bias[...]
        steps[micro, :, 0:HEADS] = jnp.maximum(shifted, 0.0) + jnp.log1p(jnp.exp(-jnp.abs(shifted)))

    row = lax.broadcasted_iota(jnp.int32, (ROWS, ROWS), 0)
    lane = lax.broadcasted_iota(jnp.int32, (ROWS, ROWS), 1)
    first_half = lane < 64
    later = row >= lane

    def states(micro):
        rates = jnp.concatenate([rate[...], jnp.zeros((1, 128 - HEADS), F32)], axis=1)
        step_size = steps[micro]
        cumulative = dot(later.astype(F32), -step_size * rates, precision=HIGHEST)
        sums[micro] = cumulative
        decay[micro] = jnp.exp(cumulative[ROWS - 1 :, :])

        @pl.when(place > 0)
        def _():
            rim(micro).wait_recv()

        for column in range(0, BOTH, 128):
            taps, at = (inner_taps, column) if column < LOCAL else (state_taps, column - LOCAL)
            total = jnp.broadcast_to(taps[TAPS, :, at : at + 128], (ROWS, 128))
            for index in range(TAPS):
                begin = EDGE - TAPS + 1 + index
                total = total + taps[index, :, at : at + 128] * (
                    padded[micro, begin : begin + ROWS, column : column + 128]
                )
            result = silu(total).astype(BF16)
            if column < LOCAL:
                inner_conv[micro, :, at : at + 128] = result
            else:
                state_conv[micro, :, at : at + 128] = result

        turned = state_conv[micro, :, 0:STATE].astype(F32).T.astype(BF16)
        for pair in range(HEADS // 2):
            heads = (2 * pair, 2 * pair + 1)
            at = slice(pair * 128, pair * 128 + 128)
            spread = [jnp.broadcast_to(cumulative[:, h : h + 1], (ROWS, 128)) for h in heads]
            sizes = [jnp.broadcast_to(step_size[:, h : h + 1], (ROWS, 128)) for h in heads]
            each = jnp.where(first_half, spread[0], spread[1])
            values = inner_conv[micro, :, at].astype(F32)
            weighting = jnp.exp(each[ROWS - 1 :, :] - each) * jnp.where(first_half, sizes[0], sizes[1])
            state = dot(turned, (values * weighting).astype(BF16))
            sent[micro, :, :, at] = state.reshape(SEQ, OWNED, 128).astype(BF16)
            growth[micro, :, at] = jnp.exp(each)

    distances = (4, 3, 5, 2, 6, 1, 7, 0)
    others = [
        lax.rem(place // 2 + step, SEQ // 2) * 2 + side
        for step in distances
        for side in range(2)
    ]

    def decay_to(micro, owner):
        return remote(
            decay.at[micro], decays.at[micro, place], decay_s.at[micro], decay_r.at[micro], {"seq": owner}
        )

    def state_to(micro, owner):
        return remote(
            sent.at[micro, owner], arrived.at[micro, place], state_s.at[micro], state_r.at[micro], {"seq": owner}
        )

    def enter_to(micro, target):
        return remote(
            back.at[micro, target], entering.at[micro, place], enter_s.at[micro], enter_r.at[micro], {"seq": target}
        )

    def all_decays(micro, count):
        block = decays.at[micro, 0:count]
        return remote(block, block, decay_s.at[micro], decay_r.at[micro], to_partner)

    def all_states(micro, count):
        block = arrived.at[micro, 0:count]
        return remote(block, block, state_s.at[micro], state_r.at[micro], to_partner)

    def all_entering(micro, count):
        block = entering.at[micro, 0:count]
        return remote(block, block, enter_s.at[micro], enter_r.at[micro], to_partner)

    def send_states(micro):
        for owner in others:

            @pl.when(jnp.logical_and(place != owner, place < SEQ - 1))
            def _():
                decay_to(micro, owner).start()
                state_to(micro, owner).start()

    def gate(micro):
        raw = (dot(xg[micro], wg[...]) * scales[micro]).astype(BF16).astype(F32)
        gate_act[micro] = silu(raw)

    def inside(micro):
        cumulative, step_size = sums[micro], steps[micro]
        across_step, across_sum = step_size.T, cumulative.T
        scores = dot_turned(state_conv[micro, :, STATE:], state_conv[micro, :, 0:STATE])
        for pair in range(HEADS // 2):
            at = slice(pair * 128, pair * 128 + 128)
            values = inner_conv[micro, :, at]
            parts = []
            for h in (2 * pair, 2 * pair + 1):
                column = jnp.broadcast_to(cumulative[:, h : h + 1], (ROWS, 128))
                fade = jnp.exp(jnp.where(later, column - across_sum[h : h + 1, :], -jnp.inf))
                mixing = (scores * fade * across_step[h : h + 1, :]).astype(BF16)
                parts.append(dot(mixing, values))
            skips = [jnp.broadcast_to(skip_scale[:, h : h + 1], (1, 128)) for h in (2 * pair, 2 * pair + 1)]
            skip = jnp.where(first_half[0:1], skips[0], skips[1])
            mixed[micro, :, at] = jnp.where(first_half, parts[0], parts[1]) + skip * values.astype(F32)

    head_of = lax.broadcasted_iota(jnp.int32, (128, LOCAL), 1) // 64
    expand = (head_of == lax.broadcasted_iota(jnp.int32, (128, LOCAL), 0)).astype(F32)

    def scan(micro):
        arrived[micro, place] = sent[micro, place]
        decays[micro, place] = decay[micro]
        @pl.when(place < SEQ - 1)
        def _():
            all_decays(micro, SEQ - 2).wait_recv()
            all_states(micro, SEQ - 2).wait_recv()

        @pl.when(place == SEQ - 1)
        def _():
            all_decays(micro, SEQ - 1).wait_recv()
            all_states(micro, SEQ - 1).wait_recv()

        rows = jnp.concatenate([decays[micro, source] for source in range(SEQ)], axis=0)
        factors = dot(rows, expand, precision=HIGHEST)
        carried = jnp.zeros((OWNED, LOCAL), F32)
        for source in range(SEQ - 1):
            carried = factors[source : source + 1, :] * carried + arrived[micro, source].astype(F32)
            back[micro, source + 1] = carried.astype(BF16)

        for target in others:

            @pl.when(jnp.logical_and(place != target, target > 0))
            def _():
                enter_to(micro, target).start()

        @pl.when(place > 0)
        def _():
            entering[micro, place] = back[micro, place]

    def across(micro):
        @pl.when(place > 0)
        def _():
            all_entering(micro, SEQ - 1).wait_recv()

        from_state = state_conv[micro, :, STATE:]
        square = jnp.zeros((ROWS, 128), F32)
        for column in range(0, LOCAL, 128):
            at = slice(column, column + 128)
            entry = entering[micro, :, :, at].astype(F32).reshape(STATE, 128).astype(BF16)
            value = mixed[micro, :, at] + growth[micro, :, at] * dot(from_state, entry)
            gated = value * gate_act[micro, :, at]
            square = square + gated * gated
            normed[micro, :, at] = (gated * inner_gain[:, at]).astype(BF16)
        return jnp.sum(square.T, axis=0, keepdims=True)

    spare_row = lax.broadcasted_iota(jnp.int32, (16, ROWS), 0)

    def split(total):
        high = total.astype(BF16).astype(F32)
        return jnp.where(spare_row < 8, high, total - high).astype(BF16)

    def half(micro, which):
        index = micro * CHIPS + which
        return remote(
            halves.at[micro, which, 1 - core], partner_half.at[micro, which], half_s.at[0], half_r.at[index],
            to_partner,
        )

    def spread(micro, total, which):
        at = pl.ds(pl.multiple_of(which * PAIR, 128), PAIR)
        product = dot(normed[micro], wo[:, at]).T
        spare = split(total)
        for side in range(2):
            halves[micro, which, side, 0:NARROW, :] = product[side * NARROW : (side + 1) * NARROW, :].astype(BF16)
            halves[micro, which, side, NARROW:SLAB, :] = spare
        half(micro, which).start()

    def unpacked(block, part):
        wide = block.astype(F32)
        if part == 0:
            return (wide,)
        rest = NARROW - HALF
        return wide[0:rest], wide[rest : rest + 1] + wide[rest + 8 : rest + 9]

    def added(*terms):
        return tuple(sum(values[1:], values[0]) for values in zip(*terms))

    def join(micro, which, part):
        rows = PARTS[part]
        return added(
            unpacked(halves[micro, which, core, rows], part), unpacked(partner_half[micro, which, rows], part)
        )

    def pack(micro, which, part, value):
        if part == 0:
            joined[micro, which, EARLY, :] = value[0].astype(BF16)
        else:
            joined[micro, which, LATE, :] = value[0].astype(BF16)
            joined[micro, which, NARROW:SLAB, :] = split(value[1])

    ways = (after, behind)

    def send_before(micro, part):
        rows, index = PARTS[part], micro * 2 + part
        return remote(
            joined.at[micro, across_ring, rows], before.at[micro, rows], before_s.at[0], before_r.at[index],
            device(ways[part]),
        )

    def send_total(micro, way, part):
        rows = PARTS[part]
        return remote(
            joined.at[micro, ways[way], rows], totals.at[micro, way, rows], total_s.at[0], total_r.at[micro],
            device(ways[way]),
        )

    def every(block, send, recv):
        return remote(block, block, send, recv, to_partner)

    def join_before(micro):
        half(micro, across_ring).wait_recv()
        for part in range(2):
            pack(micro, across_ring, part, join(micro, across_ring, part))
            send_before(micro, part).start()

    def join_direct(micro, way):
        which, part = ways[way], 1 - way
        half(micro, which).wait_recv()
        pack(micro, which, part, join(micro, which, part))
        send_total(micro, way, part).start()

    def join_second(micro):
        for part in range(2):
            which = ways[part]
            value = join(micro, which, part)
            send_before(micro, part).wait_recv()
            pack(micro, which, part, added(value, unpacked(before[micro, PARTS[part]], part)))
            send_total(micro, part, part).start()

    def finish(micro):
        half(micro, chip).wait_recv()
        values = [join(micro, chip, part) for part in range(2)]
        every(totals.at[micro], total_s.at[0], total_r.at[micro]).wait_recv()
        for way, part in ((0, 1), (1, 0), (0, 0), (1, 1)):
            values[part] = added(values[part], unpacked(totals[micro, way, PARTS[part]], part))
        scale = lax.rsqrt(values[1][1] / INNER + EPS)
        for part, rows in enumerate((EARLY, LATE)):
            result = (x[chip, micro, core, rows].astype(F32) + values[part][0] * scale).astype(BF16)
            own[micro, rows] = result
            out[0, micro, rows] = result

            @pl.when(section == 0)
            def _():
                handover(micro, part).start()

    scope = jax.named_scope
    with scope("own"):
        send_loaded(0)
        send_loaded(1)
        send_passed(0)
    for load in loads[MICRO:12]:
        load.wait()
    place_step_weights()
    with scope("near0"):
        forward_near(0)
    with scope("own1"):
        send_passed(1)
    with scope("p0"):
        project(0, chip, True)
        project(0, behind, False)

    @pl.when(section == 0)
    def _():
        forward_near(1)

    with scope("p0b"):
        project(0, after, False)
    with scope("far0"):
        forward_far(0)

    @pl.when(section == 1)
    def _():
        forward_near(1)

    with scope("far0b"):
        project(1, chip, True)
        project(0, across_ring, False)
        project_end(0)
    with scope("p1"):
        project(1, behind, False)
        project(1, after, False)
    with scope("far1"):
        forward_far(1)
        project(1, across_ring, False)
        project_end(1)
    with scope("states0"):
        states(0)
        send_states(0)
    for load in loads[12:]:
        load.wait()
    with scope("fill0"):
        gate(0)
        inside(0)
    with scope("states1"):
        states(1)
        send_states(1)
    with scope("fill1"):
        gate(1)
        inside(1)
    with scope("scan0"):
        scan(0)
    with scope("scan1"):
        scan(1)
    with scope("across0"):
        total = across(0)
    with scope("spread0"):
        spread(0, total, across_ring)
        spread(0, total, after)
        spread(0, total, behind)
        join_before(0)
    with scope("across1"):
        total1 = across(1)
    with scope("spread1"):
        spread(1, total1, across_ring)
        join_direct(0, 0)
        spread(1, total1, after)
        join_direct(0, 1)
        join_before(1)
        spread(0, total, chip)
    with scope("second0"):
        join_second(0)
        spread(1, total1, behind)
        join_direct(1, 0)
        spread(1, total1, chip)
        join_direct(1, 1)
        join_second(1)
    with scope("finish0"):
        finish(0)
    with scope("sent"):
        every(x.at[0:3, 0], gather_s.at[0], share_r.at[0]).wait_send()
        every(x.at[0:2], gather_s.at[1], share_r.at[0]).wait_send()
        for micro in range(MICRO):

            @pl.when(place < SEQ - 1)
            def _():
                rim(micro).wait_send()
                all_decays(micro, SEQ - 1).wait_send()
                all_states(micro, SEQ - 1).wait_send()

            @pl.when(place == 0)
            def _():
                all_entering(micro, SEQ - 1).wait_send()

            @pl.when(place > 0)
            def _():
                all_entering(micro, SEQ - 2).wait_send()

    with scope("finish1"):
        finish(1)

    every(halves.at[0], half_s.at[0], half_r.at[0]).wait_send()
    every(before, before_s.at[0], before_r.at[0]).wait_send()
    every(totals, total_s.at[0], total_r.at[0]).wait_send()

    @pl.when(section == 0)
    def _():
        every(own, pipe_s.at[0], pipe_r.at[0]).wait_send()


def shards(
    tokens, pre_gain, gate_w, inner_w, state_w, step_w, inner_taps, state_taps, step_bias, decay_rate, skip_scale,
    inner_gain, out_w,
):
    hbm = pl.BlockSpec(memory_space=pltpu.HBM)
    dma = lambda count: pltpu.SemaphoreType.DMA((count,))
    result = pl.pallas_call(
        kernel,
        out_shape=pltpu.VMEM((1, MICRO, NARROW, ROWS), BF16),
        in_specs=[hbm] * 13,
        out_specs=pl.BlockSpec(memory_space=pltpu.VMEM),
        scratch_shapes=[
            pltpu.VMEM((CHIPS, MICRO, 2, NARROW, ROWS), BF16),
            pltpu.VMEM((MICRO, ROWS, WIDTH), BF16),
            pltpu.VMEM((WIDTH, WIDE), BF16),
            pltpu.VMEM((HEADS, WIDTH), BF16),
            pltpu.VMEM((WIDTH, LOCAL), BF16),
            pltpu.VMEM((LOCAL, WIDTH), BF16),
            pltpu.VMEM((1, WIDTH), F32),
            pltpu.VMEM((TAPS + 1, 1, LOCAL), F32),
            pltpu.VMEM((TAPS + 1, 1, 2 * STATE), F32),
            pltpu.VMEM((1, HEADS), F32),
            pltpu.VMEM((1, HEADS), F32),
            pltpu.VMEM((1, HEADS), F32),
            pltpu.VMEM((1, LOCAL), F32),
            pltpu.VMEM((MICRO, ROWS, WIDE), F32),
            pltpu.VMEM((16, WIDTH), F32),
            pltpu.VMEM((MICRO, ROWS, LOCAL), F32),
            pltpu.VMEM((MICRO, ROWS, 128), F32),
            pltpu.VMEM((MICRO, ROWS, 1), F32),
            pltpu.VMEM((MICRO, EDGE + ROWS, BOTH), F32),
            pltpu.VMEM((MICRO, ROWS, LOCAL), BF16),
            pltpu.VMEM((MICRO, ROWS, 2 * STATE), BF16),
            pltpu.VMEM((MICRO, ROWS, 128), F32),
            pltpu.VMEM((MICRO, ROWS, 128), F32),
            pltpu.VMEM((MICRO, ROWS, LOCAL), F32),
            pltpu.VMEM((MICRO, ROWS, LOCAL), F32),
            pltpu.VMEM((MICRO, 1, 128), F32),
            pltpu.VMEM((MICRO, SEQ, 1, 128), F32),
            pltpu.VMEM((MICRO, SEQ, OWNED, LOCAL), BF16),
            pltpu.VMEM((MICRO, SEQ, OWNED, LOCAL), BF16),
            pltpu.VMEM((MICRO, SEQ, OWNED, LOCAL), BF16),
            pltpu.VMEM((MICRO, SEQ, OWNED, LOCAL), BF16),
            pltpu.VMEM((MICRO, ROWS, LOCAL), BF16),
            pltpu.VMEM((MICRO, CHIPS, 2, SLAB, ROWS), BF16),
            pltpu.VMEM((MICRO, CHIPS, SLAB, ROWS), BF16),
            pltpu.VMEM((MICRO, CHIPS, SLAB, ROWS), BF16),
            pltpu.VMEM((MICRO, SLAB, ROWS), BF16),
            pltpu.VMEM((MICRO, 2, SLAB, ROWS), BF16),
            pltpu.VMEM((MICRO, NARROW, ROWS), BF16),
            dma(14), dma(2), dma((NEAR + 1) * MICRO), dma(CHIPS * MICRO), dma(MICRO), dma(MICRO),
            dma(MICRO), dma(MICRO), dma(MICRO), dma(MICRO), dma(MICRO), dma(MICRO),
            dma(1), dma(MICRO * CHIPS), dma(1), dma(MICRO * 2), dma(1), dma(MICRO), dma(1), dma(MICRO),
        ],
        compiler_params=pltpu.CompilerParams(
            collective_id=0, has_side_effects=True, vmem_limit_bytes=56 * 1024 * 1024
        ),
    )(
        jnp.swapaxes(tokens, 1, 2), pre_gain, gate_w, inner_w, state_w, jnp.swapaxes(step_w, 1, 2),
        jnp.swapaxes(inner_taps, 0, 1), jnp.swapaxes(state_taps, 0, 1), step_bias, decay_rate, skip_scale, inner_gain,
        out_w,
    )
    return jnp.swapaxes(result, 2, 3)


def solution(mesh):
    return jax.shard_map(
        shards,
        mesh=mesh,
        in_specs=(
            P(None, "seq", "tensor"),
            P("pipe", None),
            P("pipe", None, "tensor"),
            P("pipe", None, "tensor"),
            P("pipe", None, None),
            P("pipe", None, "tensor"),
            P("pipe", None, "tensor"),
            P("pipe", None, None),
            P("pipe", "tensor"),
            P("pipe", "tensor"),
            P("pipe", "tensor"),
            P("pipe", "tensor"),
            P("pipe", "tensor", None),
        ),
        out_specs=P("pipe", None, "seq", "tensor"),
        check_vma=False,
    )
```

```python
import jax
import jax.numpy as jnp
from jax import lax
from jax.experimental import pallas as pl
from jax.experimental.pallas import tpu as pltpu
from jax.sharding import PartitionSpec as P

MESH = pl.DeviceIdType.MESH
F32, BF16 = jnp.float32, jnp.bfloat16
HIGHEST = lax.Precision.HIGHEST
EPS = 1e-05
SHARE, SEQ = 8, 16
CHIPS = SHARE // 2
MICRO, ROWS, WIDTH, INNER = 2, 128, 2560, 5120
NARROW = WIDTH // SHARE
PAIR = 2 * NARROW
LOCAL = INNER // SHARE
STATE = 128
BOTH = LOCAL + 2 * STATE
WIDE = BOTH + 128
HEADS = 10
TAPS = 4
SLAB = NARROW + 16
OWNED = STATE // SEQ
SOON = 4
EDGE = 8
HALF = NARROW // 2
SENDS = 10
NEAR = 4
EARLY, LATE = slice(0, HALF), slice(HALF, NARROW)
PARTS = (slice(0, HALF), slice(HALF, SLAB))


def silu(value):
    return value / (1.0 + jnp.exp(-value))


def dot(a, b, **options):
    return jnp.dot(a, b, preferred_element_type=F32, **options)


def dot_turned(a, b):
    return lax.dot_general(a, b, (((1,), (1,)), ((), ())), preferred_element_type=F32)


def remote(src, dst, send, recv, device):
    return pltpu.make_async_remote_copy(
        src_ref=src, dst_ref=dst, send_sem=send, recv_sem=recv, device_id=device, device_id_type=MESH
    )


def kernel(
    tokens, pre_gain_h, gate_h, inner_h, state_h, step_h, inner_taps_h, state_taps_h, bias_h, rate_h, skip_h, gain_h,
    out_h, out,
    x, xg, w1, wd, wg, wo, pre_gain, inner_taps, state_taps, bias, rate, skip_scale, inner_gain,
    acc, turned_steps, gate_act, squares, scales, padded, inner_conv, state_conv, steps, sums, growth, mixed, decay, decays, sent,
    arrived, back, entering, normed, halves, partner_half, joined, before, totals, partial, own,
    local_s, gather_s, gather_r, share_r, rim_s, rim_r, decay_s, decay_r, state_s, state_r, enter_s, enter_r, half_s, half_r,
    before_s, before_r, total_s, total_r, pipe_s, pipe_r,
):
    section, member, place = (lax.axis_index(name) for name in ("pipe", "tensor", "seq"))
    chip, core = member // 2, member % 2
    partner = member + 1 - 2 * core
    after, behind, across_ring = (lax.rem(chip + step, CHIPS) for step in (1, CHIPS - 1, 2))

    def device(which):
        return {"tensor": which * 2 + core}

    loads = [
        pltpu.make_async_copy(source, target, local_s.at[index])
        for index, (source, target) in enumerate(
            (
                (tokens.at[0], x.at[chip, 0, core]),
                (tokens.at[1], x.at[chip, 1, core]),
                (inner_h.at[0], w1.at[:, 0:LOCAL]),
                (state_h.at[0], w1.at[:, LOCAL:BOTH]),
                (step_h.at[0], wd),
                (pre_gain_h, pre_gain),
                (inner_taps_h, inner_taps),
                (state_taps_h, state_taps),
                (bias_h, bias),
                (rate_h, rate),
                (skip_h, skip_scale),
                (gain_h, inner_gain),
                (gate_h.at[0], wg),
                (out_h.at[0], wo),
            )
        )
    ]

    barrier = pltpu.get_barrier_semaphore()

    def greet(peer):
        pl.semaphore_signal(barrier, inc=1, device_id=peer, device_id_type=MESH)

    for step in range(1, SEQ):
        greet({"seq": lax.rem(place + step, SEQ)})
    greet({"pipe": 1 - section})
    greet(device(after))
    greet(device(behind))
    greet({"tensor": partner})

    @pl.when(section == 0)
    def _():
        for load in loads[:MICRO]:
            load.start()

    for load in loads[MICRO:]:
        load.start()

    steps[...] = jnp.zeros_like(steps)

    @pl.when(place == 0)
    def _():
        padded[:, 0:EDGE, :] = jnp.zeros((MICRO, EDGE, BOTH), F32)
        entering[...] = jnp.zeros_like(entering)

    pl.semaphore_wait(barrier, SEQ - 1 + 4)

    def handover(micro, part):
        rows = (EARLY, LATE)[part]
        return remote(
            own.at[micro, rows], x.at[chip, micro, core, rows], pipe_s.at[0], pipe_r.at[micro], {"pipe": 1}
        )

    def handed_over(micro):
        return remote(own.at[micro], x.at[chip, micro, core], pipe_s.at[0], pipe_r.at[micro], {"pipe": 1})

    to_partner = {"tensor": partner}

    def gather(micro, send):
        which, part, target = (
            (chip, 0, after),
            (chip, 1, behind),
            (chip, 1, after),
            (chip, 0, behind),
            (behind, 0, after),
            (after, 1, behind),
            (chip, 2, None),
            (behind, 2, None),
            (after, 2, None),
            (across_ring, 2, None),
        )[send]
        if part == 2:
            block = x.at[which, micro, core]
            return remote(block, block, gather_s.at[1], share_r.at[which * MICRO + micro], to_partner)
        block = x.at[which, micro, core, (EARLY, LATE)[part]]
        slot = NEAR * MICRO + micro if send in (4, 5) else micro * NEAR + (0, 3, 1, 2)[send]
        return remote(block, block, gather_s.at[0], gather_r.at[slot], device(target))

    def near(micro, which, part, slot):
        block = x.at[which, micro, core, (EARLY, LATE)[part]]
        return remote(block, block, gather_s.at[0], gather_r.at[micro * NEAR + slot], to_partner)

    def far(micro):
        block = x.at[across_ring, micro, core]
        return remote(block, block, gather_s.at[0], gather_r.at[NEAR * MICRO + micro], to_partner)

    def shared(micro, which):
        block = x.at[which, micro, 1 - core]
        return remote(block, block, gather_s.at[1], share_r.at[which * MICRO + micro], to_partner)

    def start_own(micro):
        for send in (0, 1, 2, 3, 6):
            gather(micro, send).start()

    def send_loaded(micro):
        @pl.when(section == 0)
        def _():
            loads[micro].wait()
            start_own(micro)

    def send_passed(micro):
        @pl.when(section == 1)
        def _():
            handed_over(micro).wait_recv()
            start_own(micro)

    def forward_near(micro):
        near(micro, behind, 0, 0).wait_recv()
        gather(micro, 4).start()
        near(micro, after, 1, 3).wait_recv()
        gather(micro, 5).start()
        near(micro, behind, 1, 1).wait_recv()
        gather(micro, 7).start()
        near(micro, after, 0, 2).wait_recv()
        gather(micro, 8).start()

    def forward_far(micro):
        far(micro).wait_recv()
        gather(micro, 9).start()

    def project(micro, which, first):
        shared(micro, which).wait_recv()
        wide = x[which, micro].reshape(PAIR, ROWS).T.astype(F32)
        at = pl.ds(pl.multiple_of(which * PAIR, 128), PAIR)
        scaled = (wide * pre_gain[:, at]).astype(BF16)
        xg[micro, :, at] = scaled
        square = wide * wide
        square = sum(square[:, column : column + 128] for column in range(0, PAIR, 128))
        term = dot(scaled, w1[at, :])
        if first:
            acc[micro], squares[micro] = term, square
        else:
            acc[micro] += term
            squares[micro] += square

    def place_step_weights():
        turned_steps[...] = jnp.zeros_like(turned_steps)
        turned_steps[0:HEADS, :] = wd[...].astype(F32)
        for column in range(0, WIDTH, 128):
            at = slice(column, column + 128)
            w1[at, BOTH : BOTH + 16] = turned_steps[:, at].T.astype(BF16)

    def rim(micro):
        return remote(
            padded.at[micro, ROWS : ROWS + EDGE, :], padded.at[micro, 0:EDGE, :], rim_s.at[micro], rim_r.at[micro],
            {"seq": lax.rem(place + 1, SEQ)},
        )

    def project_end(micro):
        scale = lax.rsqrt(jnp.sum(squares[micro], axis=1, keepdims=True) / WIDTH + EPS)
        scales[micro] = scale
        padded[micro, EDGE : EDGE + ROWS, :] = (acc[micro, :, 0:BOTH] * scale).astype(BF16).astype(F32)

        @pl.when(place < SEQ - 1)
        def _():
            rim(micro).start()

        shifted = acc[micro, :, BOTH : BOTH + HEADS] * scale + bias[...]
        steps[micro, :, 0:HEADS] = jnp.maximum(shifted, 0.0) + jnp.log1p(jnp.exp(-jnp.abs(shifted)))

    row = lax.broadcasted_iota(jnp.int32, (ROWS, ROWS), 0)
    lane = lax.broadcasted_iota(jnp.int32, (ROWS, ROWS), 1)
    first_half = lane < 64
    later = row >= lane

    distances = (4, 3, 5, 2, 6, 1, 7, 0)
    others = [
        lax.rem(place // 2 + step, SEQ // 2) * 2 + side
        for step in distances
        for side in range(2)
    ]

    def decay_to(micro, owner):
        return remote(
            decay.at[micro], decays.at[micro, place], decay_s.at[micro], decay_r.at[micro], {"seq": owner}
        )

    def prepare(micro):
        rates = jnp.concatenate([rate[...], jnp.zeros((1, 128 - HEADS), F32)], axis=1)
        step_size = steps[micro]
        cumulative = dot(later.astype(F32), -step_size * rates, precision=HIGHEST)
        sums[micro] = cumulative
        decay[micro] = jnp.exp(cumulative[ROWS - 1 :, :])
        for owner in others:

            @pl.when(jnp.logical_and(place != owner, place < SEQ - 1))
            def _():
                decay_to(micro, owner).start()

    def states(micro):
        step_size, cumulative = steps[micro], sums[micro]

        @pl.when(place > 0)
        def _():
            rim(micro).wait_recv()

        for column in range(0, BOTH, 128):
            taps, at = (inner_taps, column) if column < LOCAL else (state_taps, column - LOCAL)
            total = jnp.broadcast_to(taps[TAPS, :, at : at + 128], (ROWS, 128))
            for index in range(TAPS):
                begin = EDGE - TAPS + 1 + index
                total = total + taps[index, :, at : at + 128] * (
                    padded[micro, begin : begin + ROWS, column : column + 128]
                )
            result = silu(total).astype(BF16)
            if column < LOCAL:
                inner_conv[micro, :, at : at + 128] = result
            else:
                state_conv[micro, :, at : at + 128] = result

        turned = state_conv[micro, :, 0:STATE].astype(F32).T.astype(BF16)
        for pair in range(HEADS // 2):
            heads = (2 * pair, 2 * pair + 1)
            at = slice(pair * 128, pair * 128 + 128)
            spread = [jnp.broadcast_to(cumulative[:, h : h + 1], (ROWS, 128)) for h in heads]
            sizes = [jnp.broadcast_to(step_size[:, h : h + 1], (ROWS, 128)) for h in heads]
            each = jnp.where(first_half, spread[0], spread[1])
            values = inner_conv[micro, :, at].astype(F32)
            weighting = jnp.exp(each[ROWS - 1 :, :] - each) * jnp.where(first_half, sizes[0], sizes[1])
            state = dot(turned, (values * weighting).astype(BF16))
            sent[micro, :, :, at] = state.reshape(SEQ, OWNED, 128).astype(BF16)
            growth[micro, :, at] = jnp.exp(each)

    def state_to(micro, owner):
        return remote(
            sent.at[micro, owner], arrived.at[micro, place], state_s.at[micro],
            state_r.at[micro * 2 + jnp.minimum(place // SOON, 1)], {"seq": owner}
        )

    def enter_to(micro, target):
        return remote(
            back.at[micro, target], entering.at[micro, place], enter_s.at[micro], enter_r.at[micro], {"seq": target}
        )

    def all_decays(micro, count):
        block = decays.at[micro, 0:count]
        return remote(block, block, decay_s.at[micro], decay_r.at[micro], to_partner)

    def all_states(micro, count, group=0):
        block = arrived.at[micro, 0:count]
        return remote(block, block, state_s.at[micro], state_r.at[micro * 2 + group], to_partner)

    def all_entering(micro, count):
        block = entering.at[micro, 0:count]
        return remote(block, block, enter_s.at[micro], enter_r.at[micro], to_partner)

    def send_states(micro):
        for owner in others:

            @pl.when(jnp.logical_and(place != owner, place < SEQ - 1))
            def _():
                state_to(micro, owner).start()

    def gate(micro):
        raw = (dot(xg[micro], wg[...]) * scales[micro]).astype(BF16).astype(F32)
        gate_act[micro] = silu(raw)

    def inside(micro):
        cumulative, step_size = sums[micro], steps[micro]
        across_step, across_sum = step_size.T, cumulative.T
        scores = dot_turned(state_conv[micro, :, STATE:], state_conv[micro, :, 0:STATE])
        for pair in range(HEADS // 2):
            at = slice(pair * 128, pair * 128 + 128)
            values = inner_conv[micro, :, at]
            parts = []
            for h in (2 * pair, 2 * pair + 1):
                column = jnp.broadcast_to(cumulative[:, h : h + 1], (ROWS, 128))
                fade = jnp.exp(jnp.where(later, column - across_sum[h : h + 1, :], -jnp.inf))
                mixing = (scores * fade * across_step[h : h + 1, :]).astype(BF16)
                parts.append(dot(mixing, values))
            skips = [jnp.broadcast_to(skip_scale[:, h : h + 1], (1, 128)) for h in (2 * pair, 2 * pair + 1)]
            skip = jnp.where(first_half[0:1], skips[0], skips[1])
            mixed[micro, :, at] = jnp.where(first_half, parts[0], parts[1]) + skip * values.astype(F32)

    head_of = lax.broadcasted_iota(jnp.int32, (128, LOCAL), 1) // 64
    expand = (head_of == lax.broadcasted_iota(jnp.int32, (128, LOCAL), 0)).astype(F32)

    def scan(micro):
        arrived[micro, place] = sent[micro, place]
        decays[micro, place] = decay[micro]
        @pl.when(place < SEQ - 1)
        def _():
            all_decays(micro, SEQ - 2).wait_recv()

        @pl.when(place == SEQ - 1)
        def _():
            all_decays(micro, SEQ - 1).wait_recv()

        rows = jnp.concatenate([decays[micro, source] for source in range(SEQ)], axis=0)
        factors = dot(rows, expand, precision=HIGHEST)

        carried = jnp.zeros((OWNED, LOCAL), F32)
        for group, (begin, end) in enumerate(((0, SOON), (SOON, SEQ - 1))):
            inside_group = jnp.logical_and(place >= begin, place < end)

            @pl.when(inside_group)
            def _():
                all_states(micro, end - begin - 1, group).wait_recv()

            @pl.when(jnp.logical_not(inside_group))
            def _():
                all_states(micro, end - begin, group).wait_recv()

            for source in range(begin, end):
                carried = factors[source : source + 1, :] * carried + arrived[micro, source].astype(F32)
                back[micro, source + 1] = carried.astype(BF16)
            if group == 0:
                for target in range(1, SOON + 1):

                    @pl.when(place != target)
                    def _():
                        enter_to(micro, target).start()

        for target in others:

            @pl.when(jnp.logical_and(place != target, target > SOON))
            def _():
                enter_to(micro, target).start()

        @pl.when(place > 0)
        def _():
            entering[micro, place] = back[micro, place]

    def across(micro):
        @pl.when(place > 0)
        def _():
            all_entering(micro, SEQ - 1).wait_recv()

        from_state = state_conv[micro, :, STATE:]
        square = jnp.zeros((ROWS, 128), F32)
        for column in range(0, LOCAL, 128):
            at = slice(column, column + 128)
            entry = entering[micro, :, :, at].astype(F32).reshape(STATE, 128).astype(BF16)
            value = mixed[micro, :, at] + growth[micro, :, at] * dot(from_state, entry)
            gated = value * gate_act[micro, :, at]
            square = square + gated * gated
            normed[micro, :, at] = (gated * inner_gain[:, at]).astype(BF16)
        return jnp.sum(square.T, axis=0, keepdims=True)

    spare_row = lax.broadcasted_iota(jnp.int32, (16, ROWS), 0)

    def split(total):
        high = total.astype(BF16).astype(F32)
        return jnp.where(spare_row < 8, high, total - high).astype(BF16)

    def half(micro, which):
        index = micro * CHIPS + which
        return remote(
            halves.at[micro, which, 1 - core], partner_half.at[micro, which], half_s.at[0], half_r.at[index],
            to_partner,
        )

    def spread(micro, total, which):
        at = pl.ds(pl.multiple_of(which * PAIR, 128), PAIR)
        product = dot(normed[micro], wo[:, at]).T
        spare = split(total)
        for side in range(2):
            halves[micro, which, side, 0:NARROW, :] = product[side * NARROW : (side + 1) * NARROW, :].astype(BF16)
            halves[micro, which, side, NARROW:SLAB, :] = spare
        half(micro, which).start()

    def unpacked(block, part):
        wide = block.astype(F32)
        if part == 0:
            return (wide,)
        rest = NARROW - HALF
        return wide[0:rest], wide[rest : rest + 1] + wide[rest + 8 : rest + 9]

    def added(*terms):
        return tuple(sum(values[1:], values[0]) for values in zip(*terms))

    def join(micro, which, part):
        rows = PARTS[part]
        return added(
            unpacked(halves[micro, which, core, rows], part), unpacked(partner_half[micro, which, rows], part)
        )

    def pack(micro, which, part, value):
        if part == 0:
            joined[micro, which, EARLY, :] = value[0].astype(BF16)
        else:
            joined[micro, which, LATE, :] = value[0].astype(BF16)
            joined[micro, which, NARROW:SLAB, :] = split(value[1])

    ways = (after, behind)

    def send_before(micro, part):
        rows, index = PARTS[part], micro * 2 + part
        return remote(
            joined.at[micro, across_ring, rows], before.at[micro, rows], before_s.at[0], before_r.at[index],
            device(ways[part]),
        )

    def send_total(micro, way, part):
        rows = PARTS[part]
        return remote(
            joined.at[micro, ways[way], rows], totals.at[micro, way, rows], total_s.at[0], total_r.at[micro],
            device(ways[way]),
        )

    def every(block, send, recv):
        return remote(block, block, send, recv, to_partner)

    def join_before(micro):
        half(micro, across_ring).wait_recv()
        for part in range(2):
            pack(micro, across_ring, part, join(micro, across_ring, part))
            send_before(micro, part).start()

    def join_direct(micro, way):
        which, part = ways[way], 1 - way
        half(micro, which).wait_recv()
        pack(micro, which, part, join(micro, which, part))
        send_total(micro, way, part).start()

    def join_second(micro):
        for part in range(2):
            which = ways[part]
            value = join(micro, which, part)
            send_before(micro, part).wait_recv()
            pack(micro, which, part, added(value, unpacked(before[micro, PARTS[part]], part)))
            send_total(micro, part, part).start()

    def join_own(micro):
        half(micro, chip).wait_recv()
        values = [join(micro, chip, part) for part in range(2)]
        partial[micro, EARLY, :] = values[0][0]
        partial[micro, LATE, :] = values[1][0]
        partial[micro, NARROW : NARROW + 1, :] = values[1][1]

    def finish(micro):
        values = [(partial[micro, EARLY, :],), (partial[micro, LATE, :], partial[micro, NARROW : NARROW + 1, :])]
        every(totals.at[micro], total_s.at[0], total_r.at[micro]).wait_recv()
        for way, part in ((0, 1), (1, 0), (0, 0), (1, 1)):
            values[part] = added(values[part], unpacked(totals[micro, way, PARTS[part]], part))
        scale = lax.rsqrt(values[1][1] / INNER + EPS)
        for part, rows in enumerate((EARLY, LATE)):
            result = (x[chip, micro, core, rows].astype(F32) + values[part][0] * scale).astype(BF16)
            own[micro, rows] = result
            out[0, micro, rows] = result

            @pl.when(section == 0)
            def _():
                handover(micro, part).start()

    scope = jax.named_scope
    with scope("own"):
        send_loaded(0)
        send_loaded(1)
        send_passed(0)
    for load in loads[MICRO:12]:
        load.wait()
    place_step_weights()
    project(0, chip, True)

    @pl.when(section == 0)
    def _():
        project(1, chip, True)

    with scope("near0"):
        forward_near(0)
    with scope("own1"):
        send_passed(1)
    with scope("p0"):
        project(0, behind, False)

    @pl.when(section == 0)
    def _():
        forward_near(1)

    with scope("p0b"):
        project(0, after, False)
    with scope("far0"):
        forward_far(0)

    @pl.when(section == 1)
    def _():
        forward_near(1)
        project(1, chip, True)

    with scope("far0b"):
        project(0, across_ring, False)
        project_end(0)
    @pl.when(section == 0)
    def _():
        forward_far(1)

    with scope("p1"):
        project(1, behind, False)
        project(1, after, False)

    @pl.when(section == 1)
    def _():
        forward_far(1)

    prepare(0)
    with scope("far1"):
        project(1, across_ring, False)
        project_end(1)
    with scope("states0"):
        states(0)
        send_states(0)
    for load in loads[12:]:
        load.wait()
    with scope("fill0"):
        prepare(1)
        gate(0)
    with scope("states1"):
        states(1)
        send_states(1)
    with scope("fill1"):
        inside(0)
        gate(1)
        inside(1)
    with scope("scan0"):
        scan(0)
    with scope("scan1"):
        scan(1)
    with scope("across0"):
        total = across(0)
    with scope("spread0"):
        spread(0, total, across_ring)
        spread(0, total, after)
        spread(0, total, behind)
        join_before(0)
    with scope("across1"):
        total1 = across(1)
    with scope("spread1"):
        spread(1, total1, across_ring)
        join_direct(0, 0)
        spread(1, total1, after)
        join_direct(0, 1)
        join_before(1)
        join_second(0)
        spread(0, total, chip)
    with scope("second0"):
        spread(1, total1, behind)
        join_direct(1, 0)
        spread(1, total1, chip)
        join_direct(1, 1)
        join_own(0)
        join_own(1)
        join_second(1)
    with scope("finish0"):
        finish(0)
    with scope("sent"):
        every(x.at[0:3, 0], gather_s.at[0], share_r.at[0]).wait_send()
        every(x.at[0:2], gather_s.at[1], share_r.at[0]).wait_send()
        for micro in range(MICRO):

            @pl.when(place < SEQ - 1)
            def _():
                rim(micro).wait_send()
                all_decays(micro, SEQ - 1).wait_send()
                all_states(micro, SEQ - 1).wait_send()

            @pl.when(place == 0)
            def _():
                all_entering(micro, SEQ - 1).wait_send()

            @pl.when(place > 0)
            def _():
                all_entering(micro, SEQ - 2).wait_send()

    with scope("finish1"):
        finish(1)

    every(halves.at[0], half_s.at[0], half_r.at[0]).wait_send()
    every(before, before_s.at[0], before_r.at[0]).wait_send()
    every(totals, total_s.at[0], total_r.at[0]).wait_send()

    @pl.when(section == 0)
    def _():
        every(own, pipe_s.at[0], pipe_r.at[0]).wait_send()


def shards(
    tokens, pre_gain, gate_w, inner_w, state_w, step_w, inner_taps, state_taps, step_bias, decay_rate, skip_scale,
    inner_gain, out_w,
):
    hbm = pl.BlockSpec(memory_space=pltpu.HBM)
    dma = lambda count: pltpu.SemaphoreType.DMA((count,))
    result = pl.pallas_call(
        kernel,
        out_shape=pltpu.VMEM((1, MICRO, NARROW, ROWS), BF16),
        in_specs=[hbm] * 13,
        out_specs=pl.BlockSpec(memory_space=pltpu.VMEM),
        scratch_shapes=[
            pltpu.VMEM((CHIPS, MICRO, 2, NARROW, ROWS), BF16),
            pltpu.VMEM((MICRO, ROWS, WIDTH), BF16),
            pltpu.VMEM((WIDTH, WIDE), BF16),
            pltpu.VMEM((HEADS, WIDTH), BF16),
            pltpu.VMEM((WIDTH, LOCAL), BF16),
            pltpu.VMEM((LOCAL, WIDTH), BF16),
            pltpu.VMEM((1, WIDTH), F32),
            pltpu.VMEM((TAPS + 1, 1, LOCAL), F32),
            pltpu.VMEM((TAPS + 1, 1, 2 * STATE), F32),
            pltpu.VMEM((1, HEADS), F32),
            pltpu.VMEM((1, HEADS), F32),
            pltpu.VMEM((1, HEADS), F32),
            pltpu.VMEM((1, LOCAL), F32),
            pltpu.VMEM((MICRO, ROWS, WIDE), F32),
            pltpu.VMEM((16, WIDTH), F32),
            pltpu.VMEM((MICRO, ROWS, LOCAL), F32),
            pltpu.VMEM((MICRO, ROWS, 128), F32),
            pltpu.VMEM((MICRO, ROWS, 1), F32),
            pltpu.VMEM((MICRO, EDGE + ROWS, BOTH), F32),
            pltpu.VMEM((MICRO, ROWS, LOCAL), BF16),
            pltpu.VMEM((MICRO, ROWS, 2 * STATE), BF16),
            pltpu.VMEM((MICRO, ROWS, 128), F32),
            pltpu.VMEM((MICRO, ROWS, 128), F32),
            pltpu.VMEM((MICRO, ROWS, LOCAL), F32),
            pltpu.VMEM((MICRO, ROWS, LOCAL), F32),
            pltpu.VMEM((MICRO, 1, 128), F32),
            pltpu.VMEM((MICRO, SEQ, 1, 128), F32),
            pltpu.VMEM((MICRO, SEQ, OWNED, LOCAL), BF16),
            pltpu.VMEM((MICRO, SEQ, OWNED, LOCAL), BF16),
            pltpu.VMEM((MICRO, SEQ, OWNED, LOCAL), BF16),
            pltpu.VMEM((MICRO, SEQ, OWNED, LOCAL), BF16),
            pltpu.VMEM((MICRO, ROWS, LOCAL), BF16),
            pltpu.VMEM((MICRO, CHIPS, 2, SLAB, ROWS), BF16),
            pltpu.VMEM((MICRO, CHIPS, SLAB, ROWS), BF16),
            pltpu.VMEM((MICRO, CHIPS, SLAB, ROWS), BF16),
            pltpu.VMEM((MICRO, SLAB, ROWS), BF16),
            pltpu.VMEM((MICRO, 2, SLAB, ROWS), BF16),
            pltpu.VMEM((MICRO, NARROW + 8, ROWS), F32),
            pltpu.VMEM((MICRO, NARROW, ROWS), BF16),
            dma(14), dma(2), dma((NEAR + 1) * MICRO), dma(CHIPS * MICRO), dma(MICRO), dma(MICRO),
            dma(MICRO), dma(MICRO), dma(MICRO), dma(MICRO * 2), dma(MICRO), dma(MICRO),
            dma(1), dma(MICRO * CHIPS), dma(1), dma(MICRO * 2), dma(1), dma(MICRO), dma(1), dma(MICRO),
        ],
        compiler_params=pltpu.CompilerParams(
            collective_id=0, has_side_effects=True, vmem_limit_bytes=56 * 1024 * 1024
        ),
    )(
        jnp.swapaxes(tokens, 1, 2), pre_gain, gate_w, inner_w, state_w, jnp.swapaxes(step_w, 1, 2),
        jnp.swapaxes(inner_taps, 0, 1), jnp.swapaxes(state_taps, 0, 1), step_bias, decay_rate, skip_scale, inner_gain,
        out_w,
    )
    return jnp.swapaxes(result, 2, 3)


def solution(mesh):
    return jax.shard_map(
        shards,
        mesh=mesh,
        in_specs=(
            P(None, "seq", "tensor"),
            P("pipe", None),
            P("pipe", None, "tensor"),
            P("pipe", None, "tensor"),
            P("pipe", None, None),
            P("pipe", None, "tensor"),
            P("pipe", None, "tensor"),
            P("pipe", None, None),
            P("pipe", "tensor"),
            P("pipe", "tensor"),
            P("pipe", "tensor"),
            P("pipe", "tensor"),
            P("pipe", "tensor", None),
        ),
        out_specs=P("pipe", None, "seq", "tensor"),
        check_vma=False,
    )
```

```python
import jax
import jax.numpy as jnp
from jax import lax
from jax.experimental import pallas as pl
from jax.experimental.pallas import tpu as pltpu
from jax.sharding import PartitionSpec as P

MESH = pl.DeviceIdType.MESH
F32, BF16 = jnp.float32, jnp.bfloat16
HIGHEST = lax.Precision.HIGHEST
EPS = 1e-05
SHARE, SEQ = 8, 16
CHIPS = SHARE // 2
MICRO, ROWS, WIDTH, INNER = 2, 128, 2560, 5120
NARROW = WIDTH // SHARE
PAIR = 2 * NARROW
LOCAL = INNER // SHARE
STATE = 128
BOTH = LOCAL + 2 * STATE
WIDE = BOTH + 128
HEADS = 10
TAPS = 4
SLAB = NARROW + 16
OWNED = STATE // SEQ
SOON = 4
EDGE = 8
HALF = NARROW // 2
SENDS = 10
NEAR = 4
EARLY, LATE = slice(0, HALF), slice(HALF, NARROW)
PARTS = (slice(0, HALF), slice(HALF, SLAB))


def silu(value):
    return value / (1.0 + jnp.exp(-value))


def dot(a, b, **options):
    return jnp.dot(a, b, preferred_element_type=F32, **options)


def dot_turned(a, b):
    return lax.dot_general(a, b, (((1,), (1,)), ((), ())), preferred_element_type=F32)


def remote(src, dst, send, recv, device):
    return pltpu.make_async_remote_copy(
        src_ref=src, dst_ref=dst, send_sem=send, recv_sem=recv, device_id=device, device_id_type=MESH
    )


def kernel(
    tokens, pre_gain_h, gate_h, inner_h, state_h, step_h, inner_taps_h, state_taps_h, bias_h, rate_h, skip_h, gain_h,
    out_h, out,
    x, xg, w1, wd, wg, wo, pre_gain, inner_taps, state_taps, bias, rate, skip_scale, inner_gain,
    acc, turned_steps, gate_act, squares, scales, padded, inner_conv, state_conv, steps, sums, growth, mixed, decay, decays, sent,
    arrived, back, entering, normed, halves, partner_half, joined, before, totals, partial, own,
    local_s, gather_s, gather_r, share_r, rim_s, rim_r, decay_s, decay_r, state_s, state_r, enter_s, enter_r, half_s, half_r,
    before_s, before_r, total_s, total_r, pipe_s, pipe_r,
):
    section, member, place = (lax.axis_index(name) for name in ("pipe", "tensor", "seq"))
    chip, core = member // 2, member % 2
    partner = member + 1 - 2 * core
    after, behind, across_ring = (lax.rem(chip + step, CHIPS) for step in (1, CHIPS - 1, 2))

    def device(which):
        return {"tensor": which * 2 + core}

    loads = [
        pltpu.make_async_copy(source, target, local_s.at[index])
        for index, (source, target) in enumerate(
            (
                (tokens.at[0], x.at[chip, 0, core]),
                (tokens.at[1], x.at[chip, 1, core]),
                (inner_h.at[0], w1.at[:, 0:LOCAL]),
                (state_h.at[0], w1.at[:, LOCAL:BOTH]),
                (step_h.at[0], wd),
                (pre_gain_h, pre_gain),
                (inner_taps_h, inner_taps),
                (state_taps_h, state_taps),
                (bias_h, bias),
                (rate_h, rate),
                (skip_h, skip_scale),
                (gain_h, inner_gain),
                (gate_h.at[0], wg),
                (out_h.at[0], wo),
            )
        )
    ]

    barrier = pltpu.get_barrier_semaphore()

    def greet(peer):
        pl.semaphore_signal(barrier, inc=1, device_id=peer, device_id_type=MESH)

    for step in range(1, SEQ):
        greet({"seq": lax.rem(place + step, SEQ)})
    greet({"pipe": 1 - section})
    greet(device(after))
    greet(device(behind))
    greet({"tensor": partner})

    @pl.when(section == 0)
    def _():
        for load in loads[:MICRO]:
            load.start()

    for load in loads[MICRO:]:
        load.start()

    steps[...] = jnp.zeros_like(steps)

    @pl.when(place == 0)
    def _():
        padded[:, 0:EDGE, :] = jnp.zeros((MICRO, EDGE, BOTH), F32)
        entering[...] = jnp.zeros_like(entering)

    pl.semaphore_wait(barrier, SEQ - 1 + 4)

    def handover(micro, part):
        rows = (EARLY, LATE)[part]
        return remote(
            own.at[micro, rows], x.at[chip, micro, core, rows], pipe_s.at[0], pipe_r.at[micro], {"pipe": 1}
        )

    def handed_over(micro):
        return remote(own.at[micro], x.at[chip, micro, core], pipe_s.at[0], pipe_r.at[micro], {"pipe": 1})

    to_partner = {"tensor": partner}

    def gather(micro, send):
        which, part, target = (
            (chip, 0, after),
            (chip, 1, behind),
            (chip, 1, after),
            (chip, 0, behind),
            (behind, 0, after),
            (after, 1, behind),
            (chip, 2, None),
            (behind, 2, None),
            (after, 2, None),
            (across_ring, 2, None),
        )[send]
        if part == 2:
            block = x.at[which, micro, core]
            return remote(block, block, gather_s.at[1], share_r.at[which * MICRO + micro], to_partner)
        block = x.at[which, micro, core, (EARLY, LATE)[part]]
        slot = NEAR * MICRO + micro if send in (4, 5) else micro * NEAR + (0, 3, 1, 2)[send]
        return remote(block, block, gather_s.at[0], gather_r.at[slot], device(target))

    def near(micro, which, part, slot):
        block = x.at[which, micro, core, (EARLY, LATE)[part]]
        return remote(block, block, gather_s.at[0], gather_r.at[micro * NEAR + slot], to_partner)

    def far(micro):
        block = x.at[across_ring, micro, core]
        return remote(block, block, gather_s.at[0], gather_r.at[NEAR * MICRO + micro], to_partner)

    def shared(micro, which):
        block = x.at[which, micro, 1 - core]
        return remote(block, block, gather_s.at[1], share_r.at[which * MICRO + micro], to_partner)

    def start_own(micro):
        for send in (0, 1, 2, 3, 6):
            gather(micro, send).start()

    def send_loaded(micro):
        @pl.when(section == 0)
        def _():
            loads[micro].wait()
            start_own(micro)

    def send_passed(micro):
        @pl.when(section == 1)
        def _():
            handed_over(micro).wait_recv()
            start_own(micro)

    def forward_near(micro):
        near(micro, behind, 0, 0).wait_recv()
        gather(micro, 4).start()
        near(micro, after, 1, 3).wait_recv()
        gather(micro, 5).start()
        near(micro, behind, 1, 1).wait_recv()
        gather(micro, 7).start()
        near(micro, after, 0, 2).wait_recv()
        gather(micro, 8).start()

    def forward_far(micro):
        far(micro).wait_recv()
        gather(micro, 9).start()

    def project(micro, which, first):
        shared(micro, which).wait_recv()
        wide = x[which, micro].reshape(PAIR, ROWS).T.astype(F32)
        at = pl.ds(pl.multiple_of(which * PAIR, 128), PAIR)
        scaled = (wide * pre_gain[:, at]).astype(BF16)
        xg[micro, :, at] = scaled
        square = wide * wide
        square = sum(square[:, column : column + 128] for column in range(0, PAIR, 128))
        term = dot(scaled, w1[at, :])
        if first:
            acc[micro], squares[micro] = term, square
        else:
            acc[micro] += term
            squares[micro] += square

    def place_step_weights():
        turned_steps[...] = jnp.zeros_like(turned_steps)
        turned_steps[0:HEADS, :] = wd[...].astype(F32)
        for column in range(0, WIDTH, 128):
            at = slice(column, column + 128)
            w1[at, BOTH : BOTH + 16] = turned_steps[:, at].T.astype(BF16)

    def rim(micro):
        return remote(
            padded.at[micro, ROWS : ROWS + EDGE, :], padded.at[micro, 0:EDGE, :], rim_s.at[micro], rim_r.at[micro],
            {"seq": lax.rem(place + 1, SEQ)},
        )

    def project_end(micro):
        scale = lax.rsqrt(jnp.sum(squares[micro], axis=1, keepdims=True) / WIDTH + EPS)
        scales[micro] = scale
        padded[micro, EDGE : EDGE + ROWS, :] = (acc[micro, :, 0:BOTH] * scale).astype(BF16).astype(F32)

        @pl.when(place < SEQ - 1)
        def _():
            rim(micro).start()

        shifted = acc[micro, :, BOTH : BOTH + HEADS] * scale + bias[...]
        steps[micro, :, 0:HEADS] = jnp.maximum(shifted, 0.0) + jnp.log1p(jnp.exp(-jnp.abs(shifted)))

    row = lax.broadcasted_iota(jnp.int32, (ROWS, ROWS), 0)
    lane = lax.broadcasted_iota(jnp.int32, (ROWS, ROWS), 1)
    first_half = lane < 64
    later = row >= lane

    distances = (4, 3, 5, 2, 6, 1, 7, 0)
    others = [
        lax.rem(place // 2 + step, SEQ // 2) * 2 + side
        for step in distances
        for side in range(2)
    ]

    def decay_to(micro, owner):
        return remote(
            decay.at[micro], decays.at[micro, place], decay_s.at[micro], decay_r.at[micro], {"seq": owner}
        )

    def prepare(micro):
        rates = jnp.concatenate([rate[...], jnp.zeros((1, 128 - HEADS), F32)], axis=1)
        step_size = steps[micro]
        cumulative = dot(later.astype(F32), -step_size * rates, precision=HIGHEST)
        sums[micro] = cumulative
        decay[micro] = jnp.exp(cumulative[ROWS - 1 :, :])
        for owner in others:

            @pl.when(jnp.logical_and(place != owner, place < SEQ - 1))
            def _():
                decay_to(micro, owner).start()

    def states(micro):
        step_size, cumulative = steps[micro], sums[micro]

        @pl.when(place > 0)
        def _():
            rim(micro).wait_recv()

        for column in range(0, BOTH, 128):
            taps, at = (inner_taps, column) if column < LOCAL else (state_taps, column - LOCAL)
            total = jnp.broadcast_to(taps[TAPS, :, at : at + 128], (ROWS, 128))
            for index in range(TAPS):
                begin = EDGE - TAPS + 1 + index
                total = total + taps[index, :, at : at + 128] * (
                    padded[micro, begin : begin + ROWS, column : column + 128]
                )
            result = silu(total).astype(BF16)
            if column < LOCAL:
                inner_conv[micro, :, at : at + 128] = result
            else:
                state_conv[micro, :, at : at + 128] = result

        turned = state_conv[micro, :, 0:STATE].astype(F32).T.astype(BF16)
        for pair in range(HEADS // 2):
            heads = (2 * pair, 2 * pair + 1)
            at = slice(pair * 128, pair * 128 + 128)
            spread = [jnp.broadcast_to(cumulative[:, h : h + 1], (ROWS, 128)) for h in heads]
            sizes = [jnp.broadcast_to(step_size[:, h : h + 1], (ROWS, 128)) for h in heads]
            each = jnp.where(first_half, spread[0], spread[1])
            values = inner_conv[micro, :, at].astype(F32)
            weighting = jnp.exp(each[ROWS - 1 :, :] - each) * jnp.where(first_half, sizes[0], sizes[1])
            state = dot(turned, (values * weighting).astype(BF16))
            sent[micro, :, :, at] = state.reshape(SEQ, OWNED, 128).astype(BF16)
            growth[micro, :, at] = jnp.exp(each)

    def state_to(micro, owner):
        return remote(
            sent.at[micro, owner], arrived.at[micro, place], state_s.at[micro],
            state_r.at[micro * 3 + jnp.minimum(place // SOON, 2)], {"seq": owner}
        )

    def enter_to(micro, target):
        return remote(
            back.at[micro, target], entering.at[micro, place], enter_s.at[micro], enter_r.at[micro], {"seq": target}
        )

    def all_decays(micro, count):
        block = decays.at[micro, 0:count]
        return remote(block, block, decay_s.at[micro], decay_r.at[micro], to_partner)

    def all_states(micro, count, group=0):
        block = arrived.at[micro, 0:count]
        return remote(block, block, state_s.at[micro], state_r.at[micro * 3 + group], to_partner)

    def all_entering(micro, count):
        block = entering.at[micro, 0:count]
        return remote(block, block, enter_s.at[micro], enter_r.at[micro], to_partner)

    def send_states(micro):
        for owner in others:

            @pl.when(jnp.logical_and(place != owner, place < SEQ - 1))
            def _():
                state_to(micro, owner).start()

    def gate(micro):
        raw = (dot(xg[micro], wg[...]) * scales[micro]).astype(BF16).astype(F32)
        gate_act[micro] = silu(raw)

    def inside(micro):
        cumulative, step_size = sums[micro], steps[micro]
        across_step, across_sum = step_size.T, cumulative.T
        scores = dot_turned(state_conv[micro, :, STATE:], state_conv[micro, :, 0:STATE])
        for pair in range(HEADS // 2):
            at = slice(pair * 128, pair * 128 + 128)
            values = inner_conv[micro, :, at]
            parts = []
            for h in (2 * pair, 2 * pair + 1):
                column = jnp.broadcast_to(cumulative[:, h : h + 1], (ROWS, 128))
                fade = jnp.exp(jnp.where(later, column - across_sum[h : h + 1, :], -jnp.inf))
                mixing = (scores * fade * across_step[h : h + 1, :]).astype(BF16)
                parts.append(dot(mixing, values))
            skips = [jnp.broadcast_to(skip_scale[:, h : h + 1], (1, 128)) for h in (2 * pair, 2 * pair + 1)]
            skip = jnp.where(first_half[0:1], skips[0], skips[1])
            mixed[micro, :, at] = jnp.where(first_half, parts[0], parts[1]) + skip * values.astype(F32)

    head_of = lax.broadcasted_iota(jnp.int32, (128, LOCAL), 1) // 64
    expand = (head_of == lax.broadcasted_iota(jnp.int32, (128, LOCAL), 0)).astype(F32)

    def scan(micro):
        arrived[micro, place] = sent[micro, place]
        decays[micro, place] = decay[micro]
        @pl.when(place < SEQ - 1)
        def _():
            all_decays(micro, SEQ - 2).wait_recv()

        @pl.when(place == SEQ - 1)
        def _():
            all_decays(micro, SEQ - 1).wait_recv()

        rows = jnp.concatenate([decays[micro, source] for source in range(SEQ)], axis=0)
        factors = dot(rows, expand, precision=HIGHEST)

        carried = jnp.zeros((OWNED, LOCAL), F32)
        for group, (begin, end) in enumerate(((0, SOON), (SOON, 2 * SOON), (2 * SOON, SEQ - 1))):
            inside_group = jnp.logical_and(place >= begin, place < end)

            @pl.when(inside_group)
            def _():
                all_states(micro, end - begin - 1, group).wait_recv()

            @pl.when(jnp.logical_not(inside_group))
            def _():
                all_states(micro, end - begin, group).wait_recv()

            for source in range(begin, end):
                carried = factors[source : source + 1, :] * carried + arrived[micro, source].astype(F32)
                back[micro, source + 1] = carried.astype(BF16)
            if group < 2:
                for target in range(begin + 1, end + 1):

                    @pl.when(place != target)
                    def _():
                        enter_to(micro, target).start()

        for target in others:

            @pl.when(jnp.logical_and(place != target, target > 2 * SOON))
            def _():
                enter_to(micro, target).start()

        @pl.when(place > 0)
        def _():
            entering[micro, place] = back[micro, place]

    def across(micro):
        @pl.when(place > 0)
        def _():
            all_entering(micro, SEQ - 1).wait_recv()

        from_state = state_conv[micro, :, STATE:]
        square = jnp.zeros((ROWS, 128), F32)
        for column in range(0, LOCAL, 128):
            at = slice(column, column + 128)
            entry = entering[micro, :, :, at].astype(F32).reshape(STATE, 128).astype(BF16)
            value = mixed[micro, :, at] + growth[micro, :, at] * dot(from_state, entry)
            gated = value * gate_act[micro, :, at]
            square = square + gated * gated
            normed[micro, :, at] = (gated * inner_gain[:, at]).astype(BF16)
        return jnp.sum(square.T, axis=0, keepdims=True)

    spare_row = lax.broadcasted_iota(jnp.int32, (16, ROWS), 0)

    def split(total):
        high = total.astype(BF16).astype(F32)
        return jnp.where(spare_row < 8, high, total - high).astype(BF16)

    def half(micro, which):
        index = micro * CHIPS + which
        return remote(
            halves.at[micro, which, 1 - core], partner_half.at[micro, which], half_s.at[0], half_r.at[index],
            to_partner,
        )

    def spread(micro, total, which):
        at = pl.ds(pl.multiple_of(which * PAIR, 128), PAIR)
        product = dot(normed[micro], wo[:, at]).T
        spare = split(total)
        for side in range(2):
            halves[micro, which, side, 0:NARROW, :] = product[side * NARROW : (side + 1) * NARROW, :].astype(BF16)
            halves[micro, which, side, NARROW:SLAB, :] = spare
        half(micro, which).start()

    def unpacked(block, part):
        wide = block.astype(F32)
        if part == 0:
            return (wide,)
        rest = NARROW - HALF
        return wide[0:rest], wide[rest : rest + 1] + wide[rest + 8 : rest + 9]

    def added(*terms):
        return tuple(sum(values[1:], values[0]) for values in zip(*terms))

    def join(micro, which, part):
        rows = PARTS[part]
        return added(
            unpacked(halves[micro, which, core, rows], part), unpacked(partner_half[micro, which, rows], part)
        )

    def pack(micro, which, part, value):
        if part == 0:
            joined[micro, which, EARLY, :] = value[0].astype(BF16)
        else:
            joined[micro, which, LATE, :] = value[0].astype(BF16)
            joined[micro, which, NARROW:SLAB, :] = split(value[1])

    ways = (after, behind)

    def send_before(micro, part):
        rows, index = PARTS[part], micro * 2 + part
        return remote(
            joined.at[micro, across_ring, rows], before.at[micro, rows], before_s.at[0], before_r.at[index],
            device(ways[part]),
        )

    def send_total(micro, way, part):
        rows = PARTS[part]
        return remote(
            joined.at[micro, ways[way], rows], totals.at[micro, way, rows], total_s.at[0], total_r.at[micro],
            device(ways[way]),
        )

    def every(block, send, recv):
        return remote(block, block, send, recv, to_partner)

    def join_before(micro):
        half(micro, across_ring).wait_recv()
        for part in range(2):
            pack(micro, across_ring, part, join(micro, across_ring, part))
            send_before(micro, part).start()

    def join_direct(micro, way):
        which, part = ways[way], 1 - way
        half(micro, which).wait_recv()
        pack(micro, which, part, join(micro, which, part))
        send_total(micro, way, part).start()

    def join_second(micro):
        for part in range(2):
            which = ways[part]
            value = join(micro, which, part)
            send_before(micro, part).wait_recv()
            pack(micro, which, part, added(value, unpacked(before[micro, PARTS[part]], part)))
            send_total(micro, part, part).start()

    def join_own(micro):
        half(micro, chip).wait_recv()
        values = [join(micro, chip, part) for part in range(2)]
        partial[micro, EARLY, :] = values[0][0]
        partial[micro, LATE, :] = values[1][0]
        partial[micro, NARROW : NARROW + 1, :] = values[1][1]

    def finish(micro):
        values = [(partial[micro, EARLY, :],), (partial[micro, LATE, :], partial[micro, NARROW : NARROW + 1, :])]
        every(totals.at[micro], total_s.at[0], total_r.at[micro]).wait_recv()
        for way, part in ((0, 1), (1, 0), (0, 0), (1, 1)):
            values[part] = added(values[part], unpacked(totals[micro, way, PARTS[part]], part))
        scale = lax.rsqrt(values[1][1] / INNER + EPS)
        for part, rows in enumerate((EARLY, LATE)):
            result = (x[chip, micro, core, rows].astype(F32) + values[part][0] * scale).astype(BF16)
            own[micro, rows] = result
            out[0, micro, rows] = result

            @pl.when(section == 0)
            def _():
                handover(micro, part).start()

    scope = jax.named_scope
    with scope("own"):
        send_loaded(0)
        send_loaded(1)
        send_passed(0)
    for load in loads[MICRO:12]:
        load.wait()
    place_step_weights()
    project(0, chip, True)

    @pl.when(section == 0)
    def _():
        project(1, chip, True)

    with scope("near0"):
        forward_near(0)
    with scope("own1"):
        send_passed(1)
    with scope("p0"):
        project(0, behind, False)

    @pl.when(section == 0)
    def _():
        forward_near(1)

    with scope("p0b"):
        project(0, after, False)
    with scope("far0"):
        forward_far(0)

    @pl.when(section == 1)
    def _():
        forward_near(1)
        project(1, chip, True)

    with scope("far0b"):
        project(0, across_ring, False)
        project_end(0)
    @pl.when(section == 0)
    def _():
        forward_far(1)

    with scope("p1"):
        project(1, behind, False)
        project(1, after, False)

    @pl.when(section == 1)
    def _():
        forward_far(1)

    prepare(0)
    with scope("far1"):
        project(1, across_ring, False)
        project_end(1)
    with scope("states0"):
        states(0)
        send_states(0)
    for load in loads[12:]:
        load.wait()
    with scope("fill0"):
        prepare(1)
        gate(0)
    with scope("states1"):
        states(1)
        send_states(1)
    with scope("fill1"):
        inside(0)
        gate(1)
        inside(1)
    with scope("scan0"):
        scan(0)
    with scope("scan1"):
        scan(1)
    with scope("across0"):
        total = across(0)
    with scope("spread0"):
        spread(0, total, across_ring)
        spread(0, total, after)
        spread(0, total, behind)
        join_before(0)
    with scope("across1"):
        total1 = across(1)
    with scope("spread1"):
        spread(1, total1, across_ring)
        join_direct(0, 0)
        spread(1, total1, after)
        join_direct(0, 1)
        join_before(1)
        join_second(0)
        spread(0, total, chip)
    with scope("second0"):
        spread(1, total1, behind)
        join_direct(1, 0)
        spread(1, total1, chip)
        join_direct(1, 1)
        join_own(0)
        join_own(1)
        join_second(1)
    with scope("finish0"):
        finish(0)
    with scope("sent"):
        every(x.at[0:3, 0], gather_s.at[0], share_r.at[0]).wait_send()
        every(x.at[0:2], gather_s.at[1], share_r.at[0]).wait_send()
        for micro in range(MICRO):

            @pl.when(place < SEQ - 1)
            def _():
                rim(micro).wait_send()
                all_decays(micro, SEQ - 1).wait_send()
                all_states(micro, SEQ - 1).wait_send()

            @pl.when(place == 0)
            def _():
                all_entering(micro, SEQ - 1).wait_send()

            @pl.when(place > 0)
            def _():
                all_entering(micro, SEQ - 2).wait_send()

    with scope("finish1"):
        finish(1)

    every(halves.at[0], half_s.at[0], half_r.at[0]).wait_send()
    every(before, before_s.at[0], before_r.at[0]).wait_send()
    every(totals, total_s.at[0], total_r.at[0]).wait_send()

    @pl.when(section == 0)
    def _():
        every(own, pipe_s.at[0], pipe_r.at[0]).wait_send()


def shards(
    tokens, pre_gain, gate_w, inner_w, state_w, step_w, inner_taps, state_taps, step_bias, decay_rate, skip_scale,
    inner_gain, out_w,
):
    hbm = pl.BlockSpec(memory_space=pltpu.HBM)
    dma = lambda count: pltpu.SemaphoreType.DMA((count,))
    result = pl.pallas_call(
        kernel,
        out_shape=pltpu.VMEM((1, MICRO, NARROW, ROWS), BF16),
        in_specs=[hbm] * 13,
        out_specs=pl.BlockSpec(memory_space=pltpu.VMEM),
        scratch_shapes=[
            pltpu.VMEM((CHIPS, MICRO, 2, NARROW, ROWS), BF16),
            pltpu.VMEM((MICRO, ROWS, WIDTH), BF16),
            pltpu.VMEM((WIDTH, WIDE), BF16),
            pltpu.VMEM((HEADS, WIDTH), BF16),
            pltpu.VMEM((WIDTH, LOCAL), BF16),
            pltpu.VMEM((LOCAL, WIDTH), BF16),
            pltpu.VMEM((1, WIDTH), F32),
            pltpu.VMEM((TAPS + 1, 1, LOCAL), F32),
            pltpu.VMEM((TAPS + 1, 1, 2 * STATE), F32),
            pltpu.VMEM((1, HEADS), F32),
            pltpu.VMEM((1, HEADS), F32),
            pltpu.VMEM((1, HEADS), F32),
            pltpu.VMEM((1, LOCAL), F32),
            pltpu.VMEM((MICRO, ROWS, WIDE), F32),
            pltpu.VMEM((16, WIDTH), F32),
            pltpu.VMEM((MICRO, ROWS, LOCAL), F32),
            pltpu.VMEM((MICRO, ROWS, 128), F32),
            pltpu.VMEM((MICRO, ROWS, 1), F32),
            pltpu.VMEM((MICRO, EDGE + ROWS, BOTH), F32),
            pltpu.VMEM((MICRO, ROWS, LOCAL), BF16),
            pltpu.VMEM((MICRO, ROWS, 2 * STATE), BF16),
            pltpu.VMEM((MICRO, ROWS, 128), F32),
            pltpu.VMEM((MICRO, ROWS, 128), F32),
            pltpu.VMEM((MICRO, ROWS, LOCAL), F32),
            pltpu.VMEM((MICRO, ROWS, LOCAL), F32),
            pltpu.VMEM((MICRO, 1, 128), F32),
            pltpu.VMEM((MICRO, SEQ, 1, 128), F32),
            pltpu.VMEM((MICRO, SEQ, OWNED, LOCAL), BF16),
            pltpu.VMEM((MICRO, SEQ, OWNED, LOCAL), BF16),
            pltpu.VMEM((MICRO, SEQ, OWNED, LOCAL), BF16),
            pltpu.VMEM((MICRO, SEQ, OWNED, LOCAL), BF16),
            pltpu.VMEM((MICRO, ROWS, LOCAL), BF16),
            pltpu.VMEM((MICRO, CHIPS, 2, SLAB, ROWS), BF16),
            pltpu.VMEM((MICRO, CHIPS, SLAB, ROWS), BF16),
            pltpu.VMEM((MICRO, CHIPS, SLAB, ROWS), BF16),
            pltpu.VMEM((MICRO, SLAB, ROWS), BF16),
            pltpu.VMEM((MICRO, 2, SLAB, ROWS), BF16),
            pltpu.VMEM((MICRO, NARROW + 8, ROWS), F32),
            pltpu.VMEM((MICRO, NARROW, ROWS), BF16),
            dma(14), dma(2), dma((NEAR + 1) * MICRO), dma(CHIPS * MICRO), dma(MICRO), dma(MICRO),
            dma(MICRO), dma(MICRO), dma(MICRO), dma(MICRO * 3), dma(MICRO), dma(MICRO),
            dma(1), dma(MICRO * CHIPS), dma(1), dma(MICRO * 2), dma(1), dma(MICRO), dma(1), dma(MICRO),
        ],
        compiler_params=pltpu.CompilerParams(
            collective_id=0, has_side_effects=True, vmem_limit_bytes=56 * 1024 * 1024
        ),
    )(
        jnp.swapaxes(tokens, 1, 2), pre_gain, gate_w, inner_w, state_w, jnp.swapaxes(step_w, 1, 2),
        jnp.swapaxes(inner_taps, 0, 1), jnp.swapaxes(state_taps, 0, 1), step_bias, decay_rate, skip_scale, inner_gain,
        out_w,
    )
    return jnp.swapaxes(result, 2, 3)


def solution(mesh):
    return jax.shard_map(
        shards,
        mesh=mesh,
        in_specs=(
            P(None, "seq", "tensor"),
            P("pipe", None),
            P("pipe", None, "tensor"),
            P("pipe", None, "tensor"),
            P("pipe", None, None),
            P("pipe", None, "tensor"),
            P("pipe", None, "tensor"),
            P("pipe", None, None),
            P("pipe", "tensor"),
            P("pipe", "tensor"),
            P("pipe", "tensor"),
            P("pipe", "tensor"),
            P("pipe", "tensor", None),
        ),
        out_specs=P("pipe", None, "seq", "tensor"),
        check_vma=False,
    )
```
